32 devices in a mesh: blk: 16 (over z, y, x), sub: 2 (over core).
Axes of the slice: x: 2, y: 2, z: 4, core: 2. Of those that a mesh axis runs over, the one named last changes fastest.
Arguments:
- normal_wind: float32 [32, 55, 768], P(('blk', 'sub')), may hold values from -6 to 6
- density: float32 [32, 55, 256], P(('blk', 'sub')), may hold values from 0.5 to 1.5
- theta_field: float32 [32, 55, 256], P(('blk', 'sub')), may hold values from -6 to 6
- cell_edges: int32 [32, 6, 256], P(('blk', 'sub')), may hold values from 0 to 1663, as said below
- edge_cells: int32 [32, 2, 1664], P(('blk', 'sub')), may hold values from 0 to 703, as said below
- edges_on_edge: int32 [32, 10, 768], P(('blk', 'sub')), may hold values from 0 to 1663, as said below
- send_cells: int32 [32, 7, 64], P(('blk', 'sub')), may hold values from 0 to 255
- send_edges: int32 [32, 7, 128], P(('blk', 'sub')), may hold values from 0 to 767
- cell_weight: float32 [32, 6, 256], P(('blk', 'sub')), may hold values from -4 to 4
- eoe_weight: float32 [32, 10, 768], P(('blk', 'sub')), may hold values from -2 to 2
- vert_coupling: float32 [32, 54, 256], P(('blk', 'sub')), may hold values from 0.05 to 4
Outputs:
- density_tend: float32 [32, 55, 256], P(('blk', 'sub'))
- theta_new: float32 [32, 55, 256], P(('blk', 'sub'))
- tangential_wind: float32 [32, 55, 768], P(('blk', 'sub'))
The draws below stay inside these ranges and needn't reach their ends.
Inputs may be any that keep to these rules, and one draw needn't show every extreme that they name: `cell_edges`: positions in the block's extended edge list: owned edges, then 128 received edges for each slot in order. `edge_cells`: positions in the block's extended cell list: owned cells, then 64 received cells for each slot in order. `edges_on_edge`: positions in the block's extended edge list.
All inputs are finite; a program needn't handle non-finite values.
Results may differ from the reference program's by a relative error of at most 0.0003.
Values sent between devices are 32-bit elements; how exact they have to be, the bound alone decides.
A program may use at most 64 MiB of HBM per device.

```python
import math
import jax
import jax.numpy as jnp
from jax import lax

LEVELS = 55
CELLS_DEV = 256
EDGES_DEV = 768
HALO_CELLS = 64
HALO_EDGES = 128
SLOTS = 7
CELL_SIDES = 6
EDGE_NEIGHBOURS = 10
BLOCKS = 32
N_BLK = 16
N_SUB = 2


def live_counts(key, salt_value, capacity):
    count_key, full_key = jax.random.split(jax.random.fold_in(key, salt_value))
    counts = jax.random.randint(count_key, (BLOCKS, SLOTS), max(capacity // 4, 1), capacity + 1)
    full_slot = jax.random.randint(full_key, (BLOCKS, 1), 0, SLOTS)
    slot_ids = jnp.arange(SLOTS, dtype=jnp.int32)[None, :]
    return jnp.where(slot_ids == full_slot, capacity, counts)


def table_draw(key, salt_value, table_shape, owned, capacity, counts):
    region_key, owned_key, slot_key, entry_key = jax.random.split(jax.random.fold_in(key, salt_value), 4)
    region = jax.random.randint(region_key, table_shape, 0, 4)
    owned_pick = jax.random.randint(owned_key, table_shape, 0, owned)
    slot_pick = jax.random.randint(slot_key, table_shape, 0, SLOTS)
    slot_live = jnp.take_along_axis(counts[:, None, :], slot_pick.reshape(BLOCKS, 1, -1), axis=2).reshape(table_shape)
    entry_pick = jax.random.randint(entry_key, table_shape, 0, slot_live)
    return jnp.where(region < 3, owned_pick, owned + slot_pick * capacity + entry_pick).astype(jnp.int32)


def draw_cell_edges(key, part):
    return table_draw(key, 11, (BLOCKS, CELL_SIDES, CELLS_DEV), EDGES_DEV, HALO_EDGES, live_counts(key, 21, HALO_EDGES))


def draw_edge_cells(key, part):
    return table_draw(key, 12, (BLOCKS, 2, EDGES_DEV + SLOTS * HALO_EDGES), CELLS_DEV, HALO_CELLS, live_counts(key, 22, HALO_CELLS))


def draw_edges_on_edge(key, part):
    return table_draw(key, 13, (BLOCKS, EDGE_NEIGHBOURS, EDGES_DEV), EDGES_DEV, HALO_EDGES, live_counts(key, 21, HALO_EDGES))


def touch_ends(values, stream_key, smallest, top_value):
    spot = [jax.random.randint(jax.random.fold_in(stream_key, axis), (), 0, length) for axis, length in enumerate(values.shape)]
    main_axis = values.shape.index(max(values.shape))
    beside = spot[:main_axis] + [(spot[main_axis] + 1) % values.shape[main_axis]] + spot[main_axis + 1:]
    return values.at[tuple(spot)].set(smallest).at[tuple(beside)].set(top_value)


def shard_levels(stream_key, dims, shards, low, top_value):
    factor_of = 1.0
    for dim, shards_of in shards:
        draws = jax.random.uniform(jax.random.fold_in(jax.random.fold_in(stream_key, 6), dim), (shards_of,), jnp.float32, low / len(shards), top_value / len(shards))
        factor_of = factor_of * jnp.repeat(jnp.exp(draws), dims[dim] // shards_of).reshape((-1,) + (1,) * (len(dims) - 1 - dim))
    return factor_of


def gaussian(stream_key, shape, scale, reach, cuts=(), kind=jnp.bfloat16):
    values = scale * jax.random.normal(stream_key, shape, jnp.float32)
    if cuts:
        values = values * shard_levels(stream_key, shape, cuts, -0.22, 0.18)
    return jnp.clip(values, -reach, reach).astype(kind)


def setup_inputs(seed: int = 0) -> dict:
    arg_keys = jax.random.split(jax.random.key(seed), 12)
    normal_wind = gaussian(arg_keys[0], (BLOCKS, LEVELS, EDGES_DEV), 1.0, 6.0, ((0, 32),), jnp.float32)
    density = jnp.clip(0.5 + 1.0 * jax.random.uniform(arg_keys[1], (BLOCKS, LEVELS, CELLS_DEV), jnp.float32) ** shard_levels(arg_keys[1], (BLOCKS, LEVELS, CELLS_DEV), ((0, 32),), -0.2, 0.2), 0.5, 1.5)
    theta_field = gaussian(arg_keys[2], (BLOCKS, LEVELS, CELLS_DEV), 1.0, 6.0, ((0, 32),), jnp.float32)
    cell_edges = draw_cell_edges(jax.random.fold_in(arg_keys[11], 71), 0)
    edge_cells = draw_edge_cells(jax.random.fold_in(arg_keys[11], 71), 0)
    edges_on_edge = draw_edges_on_edge(jax.random.fold_in(arg_keys[11], 71), 0)
    send_cells = touch_ends(jax.random.randint(arg_keys[6], (BLOCKS, SLOTS, HALO_CELLS), 0, CELLS_DEV), jax.random.fold_in(arg_keys[6], 1), 0, CELLS_DEV - 1).astype(jnp.int32)
    send_edges = touch_ends(jax.random.randint(arg_keys[7], (BLOCKS, SLOTS, HALO_EDGES), 0, EDGES_DEV), jax.random.fold_in(arg_keys[7], 1), 0, EDGES_DEV - 1).astype(jnp.int32)
    cell_weight = gaussian(arg_keys[8], (BLOCKS, CELL_SIDES, CELLS_DEV), 1.0, 4.0, ((0, 32),), jnp.float32)
    eoe_weight = gaussian(arg_keys[9], (BLOCKS, EDGE_NEIGHBOURS, EDGES_DEV), EDGE_NEIGHBOURS ** -0.5, 2.0, ((0, 32),), jnp.float32)
    vert_coupling = jnp.clip(jnp.exp(math.log(4.0) - 4.3820266 * jax.random.uniform(arg_keys[10], (BLOCKS, LEVELS - 1, CELLS_DEV), jnp.float32) ** shard_levels(arg_keys[10], (BLOCKS, LEVELS - 1, CELLS_DEV), ((0, 32),), -0.2, 0.2)), 0.05, 4.0)
    return dict(normal_wind=normal_wind, density=density, theta_field=theta_field, cell_edges=cell_edges, edge_cells=edge_cells, edges_on_edge=edges_on_edge, send_cells=send_cells, send_edges=send_edges, cell_weight=cell_weight, eoe_weight=eoe_weight, vert_coupling=vert_coupling)


STEP_SIZE = 0.2
OFFSETS = (1, -1, 2, -2, 3, -3)


def column_solve(coupling, right_side):
    levels = right_side.shape[0]
    zero_row = jnp.zeros_like(right_side[0])
    ratios = []
    values = []
    ratio_prev = zero_row
    value_prev = zero_row
    for level_index in range(levels):
        coupling_below = coupling[level_index - 1] if level_index > 0 else zero_row
        coupling_above = coupling[level_index] if level_index < levels - 1 else zero_row
        divisor = 1.0 + coupling_below + coupling_above - coupling_below * ratio_prev
        ratio_now = coupling_above / divisor
        value_now = (right_side[level_index] + coupling_below * value_prev) / divisor
        ratios.append(ratio_now)
        values.append(value_now)
        ratio_prev = ratio_now
        value_prev = value_now
    result = [values[levels - 1]]
    for level_index in range(levels - 2, -1, -1):
        result.append(values[level_index] + ratios[level_index] * result[-1])
    return jnp.stack(result[::-1], axis=0)


def section_terms(density_ext, theta_ext, wind_ext, cell_edges, edge_cells, edges_on_edge, cell_weight, eoe_weight, coupling):
    owned_cells = cell_weight.shape[1]
    owned_edges = eoe_weight.shape[1]
    heat = density_ext * theta_ext
    both_ext = jnp.stack([density_ext, heat], axis=0)
    first_side = jnp.take(both_ext, edge_cells[0], axis=2)
    second_side = jnp.take(both_ext, edge_cells[1], axis=2)
    fluxes = wind_ext[None] * (0.5 * (first_side + second_side))
    density_tend = jnp.zeros((wind_ext.shape[0], owned_cells), jnp.float32)
    heat_sum = jnp.zeros((wind_ext.shape[0], owned_cells), jnp.float32)
    for side_index in range(cell_edges.shape[0]):
        weights = cell_weight[side_index]
        picked = jnp.take(fluxes, cell_edges[side_index], axis=2)
        density_tend = density_tend - weights * picked[0]
        heat_sum = heat_sum + weights * picked[1]
    theta_star = theta_ext[:, :owned_cells] - STEP_SIZE * heat_sum
    theta_new = column_solve(coupling, theta_star)
    tangential = jnp.zeros((wind_ext.shape[0], owned_edges), jnp.float32)
    for neighbour_index in range(edges_on_edge.shape[0]):
        tangential = tangential + eoe_weight[neighbour_index] * jnp.take(wind_ext, edges_on_edge[neighbour_index], axis=1)
    return density_tend, theta_new, tangential


def sender_of(block_index, slot_index):
    position = block_index // N_SUB
    side_index = block_index % N_SUB
    if slot_index < 6:
        return ((position - OFFSETS[slot_index]) % N_BLK) * N_SUB + side_index
    return position * N_SUB + (1 - side_index)


def select_block(stacked, block_index):
    return lax.dynamic_index_in_dim(stacked, block_index, 0, keepdims=False)


def extended(field, sends, block_index):
    pieces = [select_block(field, block_index)]
    for slot_index in range(7):
        source = sender_of(block_index, slot_index)
        send_rows = select_block(sends, source)[slot_index]
        source_field = select_block(field, source)
        pieces.append(jnp.take(source_field, send_rows, axis=1))
    return jnp.concatenate(pieces, axis=1)


def reference(normal_wind, density, theta_field, cell_edges, edge_cells, edges_on_edge, send_cells, send_edges, cell_weight, eoe_weight, vert_coupling):
    def one_block(block_index):
        density_ext = extended(density, send_cells, block_index)
        theta_ext = extended(theta_field, send_cells, block_index)
        wind_ext = extended(normal_wind, send_edges, block_index)
        return section_terms(density_ext, theta_ext, wind_ext, select_block(cell_edges, block_index), select_block(edge_cells, block_index), select_block(edges_on_edge, block_index), select_block(cell_weight, block_index), select_block(eoe_weight, block_index), select_block(vert_coupling, block_index))

    density_tend, theta_new, tangential = lax.map(one_block, jnp.arange(BLOCKS, dtype=jnp.int32))
    return (density_tend, theta_new, tangential)
```

```python
import functools

import jax
import jax.numpy as jnp
from jax import lax
from jax.experimental import pallas as pl
from jax.experimental.pallas import tpu as pltpu
from jax.sharding import PartitionSpec as P

STEP_SIZE = 0.2
OFFSETS = (1, -1, 2, -2, 3, -3)
SEND_ORDER = (4, 5, 2, 3, 0, 1, 6)
LANES = 128
F32 = jnp.float32
BF16 = jnp.bfloat16


def halves(values):
    lead = values.astype(BF16).astype(F32)
    return jnp.concatenate([lead, values - lead], axis=0).astype(BF16)


def dot(left, right):
    return jnp.dot(left, right, preferred_element_type=F32)


def merged_weights(indices, weights):
    total = jnp.zeros_like(weights)
    for term in range(indices.shape[0]):
        total = total + jnp.where(
            indices == indices[term : term + 1], weights[term : term + 1], 0.0
        )
    return total


def build(index_ref, weight_ref, lead_ref, trail_ref):
    terms = weight_ref.shape[0]
    row_tiles = lead_ref.shape[0] // LANES
    column_tiles = lead_ref.shape[1] // LANES

    def tile(step, carry):
        row = pl.multiple_of(lax.rem(step, row_tiles) * LANES, LANES)
        column = pl.multiple_of(lax.div(step, row_tiles) * LANES, LANES)
        columns = pl.ds(column, LANES)
        positions = lax.broadcasted_iota(jnp.int32, (LANES, LANES), 0) + row
        matrix = jnp.zeros((LANES, LANES), F32)
        for term in range(terms):
            matrix = jnp.where(
                positions == index_ref[term : term + 1, columns],
                weight_ref[term : term + 1, columns],
                matrix,
            )
        lead = matrix.astype(BF16)
        lead_ref[pl.ds(row, LANES), columns] = lead
        if trail_ref is not None:
            trail_ref[pl.ds(row, LANES), columns] = (matrix - lead.astype(F32)).astype(BF16)
        return carry

    lax.fori_loop(0, row_tiles * column_tiles, tile, 0)


def spread(indices, weights, index_ref, lead_ref, trail_ref):
    terms, outputs = indices.shape
    rows = index_ref.shape[1]
    lead = weights.astype(BF16).astype(F32)
    for term in range(terms):
        def tiled(table):
            return jnp.broadcast_to(table[term : term + 1], (rows, outputs))

        index_ref[term] = tiled(indices).astype(jnp.int16)
        lead_ref[term] = tiled(lead).astype(BF16)
        if trail_ref is not None:
            trail_ref[term] = tiled(weights - lead).astype(BF16)


def build_packed(chunk, place_ref, tables, lead_out, trail_out):
    index_ref, lead_ref, trail_ref = tables
    terms, rows = index_ref.shape[:2]
    row_tiles = lead_out.shape[0] // chunk
    column_tiles = lead_out.shape[1] // LANES

    def tile(step, carry):
        row = pl.multiple_of(lax.rem(step, row_tiles) * chunk, chunk)
        column = pl.multiple_of(lax.div(step, row_tiles) * LANES, LANES)
        columns = pl.ds(column, LANES)
        zero = jnp.zeros((rows, LANES), BF16)
        indices = [index_ref[term, :, columns] for term in range(terms)]
        leads = [lead_ref[term, :, columns] for term in range(terms)]
        if trail_out is not None:
            trails = [trail_ref[term, :, columns] for term in range(terms)]
        for part in range(chunk // rows):
            here = pl.ds(row + part * rows, rows)
            places = place_ref[here, :]
            lead, trail = zero, zero
            for term in range(terms):
                hit = places == indices[term]
                lead = jnp.where(hit, leads[term], lead)
                if trail_out is not None:
                    trail = jnp.where(hit, trails[term], trail)
            lead_out[here, columns] = lead
            if trail_out is not None:
                trail_out[here, columns] = trail
        return carry

    lax.fori_loop(0, row_tiles * column_tiles, tile, 0)


def kernel(
    wind_hbm, density_hbm, theta_hbm, cell_edges_hbm, edge_cells_hbm, edges_on_edge_hbm,
    send_cells_hbm, send_edges_hbm, cell_weight_hbm, eoe_weight_hbm, coupling_hbm,
    tend_ref, theta_new_ref, tangential_ref,
    wind_ref, density_ref, theta_ref,
    cell_edges_ref, edge_cells_ref, edges_on_edge_ref, send_cells_ref, send_edges_ref,
    cell_weight_ref, eoe_weight_ref, coupling_ref,
    wind_ext, density_ext, theta_ext, send, received,
    average, average_index, average_lead, places, diverge, diverge_trail, diverge_weight,
    tangent, tangent_trail, tangent_weight,
    average_sum, tangent_sum, inverse, carried, ratios, values,
    send_sem, recv_sem, load_sem,
):
    blocks = lax.axis_size("blk")
    position = lax.axis_index("blk")
    side = lax.axis_index("sub")
    levels, edges = tangential_ref.shape
    cells = tend_ref.shape[1]
    slots, halo_cells = send_cells_ref.shape
    halo_edges = send_edges_ref.shape[1]
    padded = wind_ext.shape[0]

    def target(slot):
        if slot < len(OFFSETS):
            return (lax.rem(position + OFFSETS[slot] + blocks, blocks), side)
        return (position, 1 - side)

    loads = (
        (send_edges_hbm, send_edges_ref),
        (wind_hbm, wind_ref),
        (send_cells_hbm, send_cells_ref),
        (density_hbm, density_ref),
        (theta_hbm, theta_ref),
        (edge_cells_hbm, edge_cells_ref),
        (cell_edges_hbm, cell_edges_ref),
        (cell_weight_hbm, cell_weight_ref),
        (edges_on_edge_hbm, edges_on_edge_ref),
        (eoe_weight_hbm, eoe_weight_ref),
        (coupling_hbm, coupling_ref),
    )
    loads = [
        pltpu.make_async_copy(
            source.at[0] if source is edge_cells_hbm else source.at[:, 0, :], target_ref, load_sem.at[n]
        )
        for n, (source, target_ref) in enumerate(loads)
    ]
    for load in loads:
        load.start()

    barrier = pltpu.get_barrier_semaphore()
    for slot in range(slots):
        pl.semaphore_signal(
            barrier, inc=1, device_id=target(slot), device_id_type=pl.DeviceIdType.MESH
        )

    for load in loads[:5]:
        load.wait()
    for ext, ref in ((wind_ext, wind_ref), (density_ext, density_ref), (theta_ext, theta_ref)):
        owned = ref.shape[1]
        ext[0:levels, 0:owned] = ref[...]
        if levels < padded:
            ext[levels:padded, 0:owned] = jnp.zeros((padded - levels, owned), F32)
    spare = cells + slots * halo_cells
    for ext in (density_ext, theta_ext):
        if spare < ext.shape[1]:
            ext[:, spare:] = jnp.zeros((padded, ext.shape[1] - spare), F32)

    wind_own = halves(wind_ext[:, 0:edges])
    cells_own = halves(
        jnp.concatenate([density_ext[:, 0:cells], theta_ext[:, 0:cells]], axis=0)
    )

    edge_rows = lax.broadcasted_iota(jnp.int32, (edges, halo_edges), 0)
    cell_rows = lax.broadcasted_iota(jnp.int32, (cells, halo_cells), 0)
    for slot in range(slots):
        picks = jnp.where(edge_rows == send_edges_ref[slot : slot + 1, :], 1.0, 0.0).astype(BF16)
        both = dot(wind_own, picks)
        send[slot, :, 2 * halo_cells :] = both[0:padded] + both[padded:]
        picks = jnp.where(cell_rows == send_cells_ref[slot : slot + 1, :], 1.0, 0.0).astype(BF16)
        both = dot(cells_own, picks)
        both = both[0 : 2 * padded] + both[2 * padded :]
        send[slot, :, 0:halo_cells] = both[0:padded]
        send[slot, :, halo_cells : 2 * halo_cells] = both[padded:]

    def copy_of(slot):
        return pltpu.make_async_remote_copy(
            src_ref=send.at[slot],
            dst_ref=received.at[slot],
            send_sem=send_sem.at[slot],
            recv_sem=recv_sem.at[slot],
            device_id=target(slot),
            device_id_type=pl.DeviceIdType.MESH,
        )

    pl.semaphore_wait(barrier, slots)
    for slot in SEND_ORDER:
        copy_of(slot).start()

    for load in loads[5:]:
        load.wait()
    tangent_weight[...] = merged_weights(edges_on_edge_ref[...], eoe_weight_ref[...])
    diverge_weight[...] = merged_weights(cell_edges_ref[...], cell_weight_ref[...])
    average_tables = (average_index, average_lead, None)
    spread(
        edge_cells_ref[...],
        merged_weights(edge_cells_ref[...], jnp.full(edge_cells_ref.shape, 0.5, F32)),
        *average_tables,
    )
    places[...] = lax.broadcasted_iota(jnp.int32, places.shape, 0).astype(jnp.int16)
    build_packed(average.shape[0], places, average_tables, average, None)
    build(cell_edges_ref, diverge_weight, diverge, diverge_trail)
    build(edges_on_edge_ref, tangent_weight, tangent, tangent_trail)

    ratio = jnp.zeros((1, cells), F32)
    below = jnp.zeros((1, cells), F32)
    for level in range(levels):
        if level < levels - 1:
            above = coupling_ref[level : level + 1, :]
        else:
            above = jnp.zeros((1, cells), F32)
        reciprocal = 1.0 / (1.0 + below + above - below * ratio)
        ratio = above * reciprocal
        inverse[level : level + 1, :] = reciprocal
        carried[level : level + 1, :] = below * reciprocal
        ratios[level : level + 1, :] = ratio
        below = above

    wind_own = halves(wind_ext[:, 0:edges])
    both = dot(wind_own, tangent[0:edges, :])
    tangent_sum[...] = both[0:padded] + both[padded:] + dot(
        wind_own[0:padded], tangent_trail[0:edges, :]
    )
    own = density_ext[:, 0:cells]
    both = dot(
        halves(jnp.concatenate([own, own * theta_ext[:, 0:cells]], axis=0)),
        average[0:cells, :],
    )
    average_sum[...] = both[0 : 2 * padded] + both[2 * padded :]

    for slot in SEND_ORDER:
        copy_of(slot).wait_recv()
    for slot in range(slots):
        start = cells + slot * halo_cells
        density_ext[:, start : start + halo_cells] = received[slot, :, 0:halo_cells]
        theta_ext[:, start : start + halo_cells] = received[slot, :, halo_cells : 2 * halo_cells]
        start = edges + slot * halo_edges
        wind_ext[:, start : start + halo_edges] = received[slot, :, 2 * halo_cells :]

    halo = density_ext[:, cells:]
    both = dot(
        halves(jnp.concatenate([halo, halo * theta_ext[:, cells:]], axis=0)),
        average[cells:, :],
    )
    averaged = average_sum[...] + both[0 : 2 * padded] + both[2 * padded :]
    wind = wind_ext[...]
    fluxes = halves(jnp.concatenate([wind, wind], axis=0) * averaged)
    both = dot(fluxes, diverge[...])
    divergence = both[0 : 2 * padded] + both[2 * padded :] + dot(
        fluxes[0 : 2 * padded], diverge_trail[...]
    )
    tend_ref[...] = -divergence[0:levels]
    values[...] = (theta_ext[:, 0:cells] - STEP_SIZE * divergence[padded:])
    values[0:levels, :] = values[0:levels, :] * inverse[0:levels, :]

    wind_halo = halves(wind_ext[:, edges:])
    both = dot(wind_halo, tangent[edges:, :])
    tangential = tangent_sum[...] + both[0:padded] + both[padded:] + dot(
        wind_halo[0:padded], tangent_trail[edges:, :]
    )
    tangential_ref[...] = tangential[0:levels]

    value = jnp.zeros((1, cells), F32)
    for level in range(levels):
        value = values[level : level + 1, :] + carried[level : level + 1, :] * value
        values[level : level + 1, :] = value
    theta_new_ref[levels - 1 : levels, :] = value
    for level in range(levels - 2, -1, -1):
        value = values[level : level + 1, :] + ratios[level : level + 1, :] * value
        theta_new_ref[level : level + 1, :] = value

    for slot in SEND_ORDER:
        copy_of(slot).wait_send()


def deliver(*refs):
    sources, targets, store_sem = refs[:3], refs[3:6], refs[6]
    stores = [
        pltpu.make_async_copy(source, target_ref.at[:, 0, :], store_sem.at[n])
        for n, (source, target_ref) in enumerate(zip(sources, targets))
    ]
    for store in stores:
        store.start()
    for store in stores:
        store.wait()


def spread_of(table):
    shape = (table.shape[1], 16, table.shape[2])
    return [pltpu.VMEM(shape, kind) for kind in (jnp.int16, BF16, BF16)]


def shards(*arguments):
    wind, density, theta, cell_edges, edge_cells, edges_on_edge, send_cells, send_edges = arguments[:8]
    levels, edges = wind.shape[1:]
    cells = density.shape[2]
    slots, halo_cells = send_cells.shape[1:]
    halo_edges = send_edges.shape[2]
    padded = -(-levels // 8) * 8
    edges_ext = edge_cells.shape[2]
    cells_ext = -(-(cells + slots * halo_cells) // LANES) * LANES
    landed = [*arguments[:3], cell_edges, edge_cells, edges_on_edge, send_cells, send_edges, *arguments[8:]]
    operands = [x if x is edge_cells else jnp.transpose(x, (1, 0, 2)) for x in arguments]
    hbm = pl.BlockSpec(memory_space=pl.ANY)
    vmem = pl.BlockSpec(memory_space=pltpu.VMEM)
    widths = (cells, cells, edges)
    results = pl.pallas_call(
        kernel,
        out_shape=tuple(pltpu.VMEM((levels, width), F32) for width in widths),
        in_specs=[hbm] * len(arguments),
        out_specs=(vmem,) * 3,
        scratch_shapes=[
            *(pltpu.VMEM(x.shape[1:], x.dtype) for x in landed),
            pltpu.VMEM((padded, edges_ext), F32),
            pltpu.VMEM((padded, cells_ext), F32),
            pltpu.VMEM((padded, cells_ext), F32),
            pltpu.VMEM((slots, padded, 2 * halo_cells + halo_edges), F32),
            pltpu.VMEM((slots, padded, 2 * halo_cells + halo_edges), F32),
            pltpu.VMEM((cells_ext, edges_ext), BF16),
            *spread_of(edge_cells)[:2],
            pltpu.VMEM((cells_ext, LANES), jnp.int16),
            pltpu.VMEM((edges_ext, cells), BF16),
            pltpu.VMEM((edges_ext, cells), BF16),
            pltpu.VMEM(cell_edges.shape[1:], F32),
            pltpu.VMEM((edges_ext, edges), BF16),
            pltpu.VMEM((edges_ext, edges), BF16),
            pltpu.VMEM(edges_on_edge.shape[1:], F32),
            pltpu.VMEM((2 * padded, edges_ext), F32),
            pltpu.VMEM((padded, edges), F32),
            pltpu.VMEM((padded, cells), F32),
            pltpu.VMEM((padded, cells), F32),
            pltpu.VMEM((padded, cells), F32),
            pltpu.VMEM((padded, cells), F32),
            pltpu.SemaphoreType.DMA((slots,)),
            pltpu.SemaphoreType.DMA((slots,)),
            pltpu.SemaphoreType.DMA((len(arguments),)),
        ],
        compiler_params=pltpu.CompilerParams(collective_id=0, has_side_effects=True),
    )(*operands)
    results = pl.pallas_call(
        deliver,
        out_shape=tuple(jax.ShapeDtypeStruct((levels, 1, width), F32) for width in widths),
        in_specs=[vmem] * 3,
        out_specs=(hbm,) * 3,
        scratch_shapes=[pltpu.SemaphoreType.DMA((3,))],
    )(*(pltpu.with_memory_space_constraint(x, pltpu.VMEM) for x in results))
    return tuple(jnp.transpose(x, (1, 0, 2)) for x in results)


def solution(mesh):
    placed = P(("blk", "sub"), None, None)
    return jax.shard_map(
        shards,
        mesh=mesh,
        in_specs=(placed,) * 11,
        out_specs=(placed,) * 3,
        check_vma=False,
    )
```

```python
import functools

import jax
import jax.numpy as jnp
from jax import lax
from jax.experimental import pallas as pl
from jax.experimental.pallas import tpu as pltpu
from jax.sharding import PartitionSpec as P

STEP_SIZE = 0.2
OFFSETS = (1, -1, 2, -2, 3, -3)
SEND_ORDER = (4, 5, 2, 3, 0, 1, 6)
WRAP_ORDERS = {
    -1: (0, 2, 4, 5, 3, 1, 6),
    -2: (2, 4, 5, 3, 0, 1, 6),
    0: (1, 3, 5, 4, 2, 0, 6),
    1: (3, 5, 4, 2, 0, 1, 6),
    2: (5, 4, 3, 2, 0, 1, 6),
}
URGENT = 3
LANES = 128
F32 = jnp.float32
BF16 = jnp.bfloat16


def halves(values):
    lead = values.astype(BF16).astype(F32)
    return jnp.concatenate([lead, values - lead], axis=0).astype(BF16)


def dot(left, right):
    return jnp.dot(left, right, preferred_element_type=F32)


def merged_weights(indices, weights):
    total = jnp.zeros_like(weights)
    for term in range(indices.shape[0]):
        total = total + jnp.where(
            indices == indices[term : term + 1], weights[term : term + 1], 0.0
        )
    return total


def moved(indices, owned, halo, shifts):
    shift = jnp.zeros_like(indices)
    for slot, amount in enumerate(shifts):
        shift = jnp.where(indices >= owned + slot * halo, amount * halo, shift)
    return indices + shift


def build(index_ref, weight_ref, lead_ref, trail_ref, first=0, last=None):
    terms = weight_ref.shape[0]
    row_tiles = lead_ref.shape[0] // LANES
    column_tiles = lead_ref.shape[1] // LANES

    def tile(step, carry):
        row = pl.multiple_of(lax.rem(step, row_tiles) * LANES, LANES)
        column = pl.multiple_of(lax.div(step, row_tiles) * LANES, LANES)
        columns = pl.ds(column, LANES)
        positions = lax.broadcasted_iota(jnp.int32, (LANES, LANES), 0) + row
        matrix = jnp.zeros((LANES, LANES), F32)
        for term in range(terms):
            matrix = jnp.where(
                positions == index_ref[term : term + 1, columns],
                weight_ref[term : term + 1, columns],
                matrix,
            )
        lead = matrix.astype(BF16)
        lead_ref[pl.ds(row, LANES), columns] = lead
        if trail_ref is not None:
            trail_ref[pl.ds(row, LANES), columns] = (matrix - lead.astype(F32)).astype(BF16)
        return carry

    lax.fori_loop(first, row_tiles * column_tiles if last is None else last, tile, 0)


def spread(indices, weights, index_ref, lead_ref, trail_ref):
    terms, outputs = indices.shape
    rows = index_ref.shape[1]
    lead = weights.astype(BF16).astype(F32)
    for term in range(terms):
        def tiled(table):
            return jnp.broadcast_to(table[term : term + 1], (rows, outputs))

        index_ref[term] = tiled(indices).astype(jnp.int16)
        lead_ref[term] = tiled(lead).astype(BF16)
        if trail_ref is not None:
            trail_ref[term] = tiled(weights - lead).astype(BF16)


def build_packed(chunk, place_ref, tables, lead_out, trail_out):
    index_ref, lead_ref, trail_ref = tables
    terms, rows = index_ref.shape[:2]
    row_tiles = lead_out.shape[0] // chunk
    column_tiles = lead_out.shape[1] // LANES

    def tile(step, carry):
        row = pl.multiple_of(lax.rem(step, row_tiles) * chunk, chunk)
        column = pl.multiple_of(lax.div(step, row_tiles) * LANES, LANES)
        columns = pl.ds(column, LANES)
        zero = jnp.zeros((rows, LANES), BF16)
        indices = [index_ref[term, :, columns] for term in range(terms)]
        leads = [lead_ref[term, :, columns] for term in range(terms)]
        if trail_out is not None:
            trails = [trail_ref[term, :, columns] for term in range(terms)]
        for part in range(chunk // rows):
            here = pl.ds(row + part * rows, rows)
            places = place_ref[here, :]
            lead, trail = zero, zero
            for term in range(terms):
                hit = places == indices[term]
                lead = jnp.where(hit, leads[term], lead)
                if trail_out is not None:
                    trail = jnp.where(hit, trails[term], trail)
            lead_out[here, columns] = lead
            if trail_out is not None:
                trail_out[here, columns] = trail
        return carry

    lax.fori_loop(0, row_tiles * column_tiles, tile, 0)


def kernel(
    wind_hbm, density_hbm, theta_hbm, cell_edges_hbm, edge_cells_hbm, edges_on_edge_hbm,
    send_cells_hbm, send_edges_hbm, cell_weight_hbm, eoe_weight_hbm, coupling_hbm,
    tend_ref, theta_new_ref, tangential_ref,
    wind_ref, density_ref, theta_ref,
    cell_edges_ref, edge_cells_ref, edges_on_edge_ref, send_cells_ref, send_edges_ref,
    cell_weight_ref, eoe_weight_ref, coupling_ref,
    wind_ext, density_ext, theta_ext, send, received,
    average, average_index, average_lead, places, diverge, diverge_trail, diverge_weight,
    tangent, tangent_trail, tangent_weight,
    average_sum, tangent_sum, inverse, carried, ratios, values,
    send_sem, recv_sem, load_sem,
):
    blocks = lax.axis_size("blk")
    position = lax.axis_index("blk")
    side = lax.axis_index("sub")
    levels, edges = tangential_ref.shape
    cells = tend_ref.shape[1]
    slots, halo_cells = send_cells_ref.shape
    halo_edges = send_edges_ref.shape[1]
    padded = wind_ext.shape[0]

    def target(slot):
        if isinstance(slot, int):
            if slot == len(OFFSETS):
                return (position, 1 - side)
            return (lax.rem(position + OFFSETS[slot] + blocks, blocks), side)
        offset = (lax.div(slot, 2) + 1) * (1 - 2 * lax.rem(slot, 2))
        across = slot == len(OFFSETS)
        offset = jnp.where(across, 0, offset)
        return (lax.rem(position + offset + blocks, blocks), jnp.where(across, 1 - side, side))

    barrier = pltpu.get_barrier_semaphore()
    for slot in SEND_ORDER:
        pl.semaphore_signal(
            barrier, inc=1, device_id=target(slot), device_id_type=pl.DeviceIdType.MESH
        )

    loads = (
        (send_edges_hbm, send_edges_ref),
        (wind_hbm, wind_ref),
        (send_cells_hbm, send_cells_ref),
        (density_hbm, density_ref),
        (theta_hbm, theta_ref),
        (edge_cells_hbm, edge_cells_ref),
        (cell_edges_hbm, cell_edges_ref),
        (cell_weight_hbm, cell_weight_ref),
        (edges_on_edge_hbm, edges_on_edge_ref),
        (eoe_weight_hbm, eoe_weight_ref),
        (coupling_hbm, coupling_ref),
    )
    loads = [
        pltpu.make_async_copy(
            source.at[0] if source is edge_cells_hbm else source.at[:, 0, :], target_ref, load_sem.at[n]
        )
        for n, (source, target_ref) in enumerate(loads)
    ]
    for load in loads:
        load.start()

    for load in loads[:5]:
        load.wait()
    for ext, ref in ((wind_ext, wind_ref), (density_ext, density_ref), (theta_ext, theta_ref)):
        owned = ref.shape[1]
        ext[0:levels, 0:owned] = ref[...]
        if levels < padded:
            ext[levels:padded, 0:owned] = jnp.zeros((padded - levels, owned), F32)
    spare = cells + slots * halo_cells
    for ext in (density_ext, theta_ext):
        if spare < ext.shape[1]:
            ext[:, spare:] = jnp.zeros((padded, ext.shape[1] - spare), F32)

    upper = 2 * position >= blocks
    parity = jnp.where(upper, 1, 0)
    rank = [
        jnp.where(parity == slot % 2, 4 + slot // 2, 1 + slot // 2) for slot in range(len(OFFSETS))
    ] + [0]
    shifts = [rank[slot] - slot for slot in range(slots)]

    order = []
    for step, slot in enumerate(SEND_ORDER):
        for place, slots_there in WRAP_ORDERS.items():
            slot = jnp.where(position == lax.rem(place + blocks, blocks), slots_there[step], slot)
        order.append(slot)

    edge_rows = lax.broadcasted_iota(jnp.int32, (edges, halo_edges), 0)
    cell_rows = lax.broadcasted_iota(jnp.int32, (cells, halo_cells), 0)

    def gather(some):
        wind_own = halves(wind_ext[:, 0:edges])
        cells_own = halves(
            jnp.concatenate([density_ext[:, 0:cells], theta_ext[:, 0:cells]], axis=0)
        )
        for slot in some:
            row = pl.ds(slot, 1)
            picks = jnp.where(edge_rows == send_edges_ref[row, :], 1.0, 0.0).astype(BF16)
            both = dot(wind_own, picks)
            send[slot, :, 2 * halo_cells :] = both[0:padded] + both[padded:]
            picks = jnp.where(cell_rows == send_cells_ref[row, :], 1.0, 0.0).astype(BF16)
            both = dot(cells_own, picks)
            both = both[0 : 2 * padded] + both[2 * padded :]
            send[slot, :, 0:halo_cells] = both[0:padded]
            send[slot, :, halo_cells : 2 * halo_cells] = both[padded:]

    def copy_of(slot):
        return pltpu.make_async_remote_copy(
            src_ref=send.at[slot],
            dst_ref=received.at[slot],
            send_sem=send_sem.at[slot],
            recv_sem=recv_sem.at[slot],
            device_id=target(slot),
            device_id_type=pl.DeviceIdType.MESH,
        )

    def prepare_tangent():
        indices = moved(edges_on_edge_ref[...], edges, halo_edges, shifts)
        tangent_weight[...] = merged_weights(indices, eoe_weight_ref[...])
        edges_on_edge_ref[...] = indices

    tangent_steps = (tangent.shape[0] // LANES) * (tangent.shape[1] // LANES)
    tangent_ahead = jnp.where(
        position == 0, 5 * tangent_steps // 6, jnp.where(position < 3, tangent_steps // 2, 0)
    )
    early = position < 3

    gather(order[:URGENT])
    for load in loads[5:]:
        load.wait()

    @pl.when(early)
    def _():
        gather(order[URGENT:])
        prepare_tangent()
        build(edges_on_edge_ref, tangent_weight, tangent, tangent_trail, 0, tangent_ahead)

    pl.semaphore_wait(barrier, slots)
    for slot in order[:URGENT]:
        copy_of(slot).start()

    @pl.when(jnp.logical_not(early))
    def _():
        gather(order[URGENT:])

    for slot in order[URGENT:]:
        copy_of(slot).start()

    @pl.when(jnp.logical_not(early))
    def _():
        prepare_tangent()

    indices = moved(cell_edges_ref[...], edges, halo_edges, shifts)
    diverge_weight[...] = merged_weights(indices, cell_weight_ref[...])
    cell_edges_ref[...] = indices
    average_tables = (average_index, average_lead, None)
    indices = moved(edge_cells_ref[...], cells, halo_cells, shifts)
    edge_cells_ref[:, 0:edges] = indices[:, 0:edges]
    for slot in range(slots):
        start = edges + slot * halo_edges
        place = pl.multiple_of(edges + rank[slot] * halo_edges, LANES)
        edge_cells_ref[:, pl.ds(place, halo_edges)] = indices[:, start : start + halo_edges]
    indices = edge_cells_ref[...]
    spread(
        indices,
        merged_weights(indices, jnp.full(edge_cells_ref.shape, 0.5, F32)),
        *average_tables,
    )
    places[...] = lax.broadcasted_iota(jnp.int32, places.shape, 0).astype(jnp.int16)
    build_packed(average.shape[0], places, average_tables, average, None)
    build(cell_edges_ref, diverge_weight, diverge, diverge_trail)
    build(
        edges_on_edge_ref, tangent_weight, tangent, tangent_trail, tangent_ahead, tangent_steps
    )

    ratio = jnp.zeros((1, cells), F32)
    below = jnp.zeros((1, cells), F32)
    for level in range(levels):
        if level < levels - 1:
            above = coupling_ref[level : level + 1, :]
        else:
            above = jnp.zeros((1, cells), F32)
        reciprocal = 1.0 / (1.0 + below + above - below * ratio)
        ratio = above * reciprocal
        inverse[level : level + 1, :] = reciprocal
        carried[level : level + 1, :] = below * reciprocal
        ratios[level : level + 1, :] = ratio
        below = above

    def tangent_part(lower, higher):
        part = halves(wind_ext[:, lower:higher])
        both = dot(part, tangent[lower:higher, :])
        return both[0:padded] + both[padded:] + dot(
            part[0:padded], tangent_trail[lower:higher, :]
        )

    def average_part(lower, higher):
        part = density_ext[:, lower:higher]
        both = dot(
            halves(jnp.concatenate([part, part * theta_ext[:, lower:higher]], axis=0)),
            average[lower:higher, :],
        )
        return both[0 : 2 * padded] + both[2 * padded :]

    def take(slot, place):
        copy_of(slot).wait_recv()
        start = cells + place * halo_cells
        density_ext[:, start : start + halo_cells] = received[slot, :, 0:halo_cells]
        theta_ext[:, start : start + halo_cells] = received[slot, :, halo_cells : 2 * halo_cells]
        start = edges + place * halo_edges
        wind_ext[:, start : start + halo_edges] = received[slot, :, 2 * halo_cells :]

    tangent_sum[...] = tangent_part(0, edges)
    average_sum[...] = average_part(0, cells)

    near = 1 + len(OFFSETS) // 2
    take(slots - 1, 0)
    for pair in range(near - 1):
        take(2 * pair + 1 - parity, 1 + pair)
    edges_near, cells_near = edges + near * halo_edges, cells + near * halo_cells
    tangent_sum[...] += tangent_part(edges, edges_near)
    average_sum[...] += average_part(cells, cells_near)

    for pair in range(near - 1):
        take(2 * pair + parity, near + pair)
    averaged = average_sum[...] + average_part(cells_near, density_ext.shape[1])
    wind = wind_ext[...]
    fluxes = halves(jnp.concatenate([wind, wind], axis=0) * averaged)
    both = dot(fluxes, diverge[...])
    divergence = both[0 : 2 * padded] + both[2 * padded :] + dot(
        fluxes[0 : 2 * padded], diverge_trail[...]
    )
    tend_ref[...] = -divergence[0:levels]
    values[...] = (theta_ext[:, 0:cells] - STEP_SIZE * divergence[padded:])
    values[0:levels, :] = values[0:levels, :] * inverse[0:levels, :]

    tangential = tangent_sum[...] + tangent_part(edges_near, wind_ext.shape[1])
    tangential_ref[...] = tangential[0:levels]

    value = jnp.zeros((1, cells), F32)
    for level in range(levels):
        value = values[level : level + 1, :] + carried[level : level + 1, :] * value
        values[level : level + 1, :] = value
    theta_new_ref[levels - 1 : levels, :] = value
    for level in range(levels - 2, -1, -1):
        value = values[level : level + 1, :] + ratios[level : level + 1, :] * value
        theta_new_ref[level : level + 1, :] = value

    for slot in SEND_ORDER:
        copy_of(slot).wait_send()


def deliver(*refs):
    sources, targets, store_sem = refs[:3], refs[3:6], refs[6]
    stores = [
        pltpu.make_async_copy(source, target_ref.at[:, 0, :], store_sem.at[n])
        for n, (source, target_ref) in enumerate(zip(sources, targets))
    ]
    for store in stores:
        store.start()
    for store in stores:
        store.wait()


def spread_of(table):
    shape = (table.shape[1], 16, table.shape[2])
    return [pltpu.VMEM(shape, kind) for kind in (jnp.int16, BF16, BF16)]


def shards(*arguments):
    wind, density, theta, cell_edges, edge_cells, edges_on_edge, send_cells, send_edges = arguments[:8]
    levels, edges = wind.shape[1:]
    cells = density.shape[2]
    slots, halo_cells = send_cells.shape[1:]
    halo_edges = send_edges.shape[2]
    padded = -(-levels // 8) * 8
    edges_ext = edge_cells.shape[2]
    cells_ext = -(-(cells + slots * halo_cells) // LANES) * LANES
    landed = [*arguments[:3], cell_edges, edge_cells, edges_on_edge, send_cells, send_edges, *arguments[8:]]
    operands = [x if x is edge_cells else jnp.transpose(x, (1, 0, 2)) for x in arguments]
    hbm = pl.BlockSpec(memory_space=pl.ANY)
    vmem = pl.BlockSpec(memory_space=pltpu.VMEM)
    widths = (cells, cells, edges)
    results = pl.pallas_call(
        kernel,
        out_shape=tuple(pltpu.VMEM((levels, width), F32) for width in widths),
        in_specs=[hbm] * len(arguments),
        out_specs=(vmem,) * 3,
        scratch_shapes=[
            *(pltpu.VMEM(x.shape[1:], x.dtype) for x in landed),
            pltpu.VMEM((padded, edges_ext), F32),
            pltpu.VMEM((padded, cells_ext), F32),
            pltpu.VMEM((padded, cells_ext), F32),
            pltpu.VMEM((slots, padded, 2 * halo_cells + halo_edges), F32),
            pltpu.VMEM((slots, padded, 2 * halo_cells + halo_edges), F32),
            pltpu.VMEM((cells_ext, edges_ext), BF16),
            *spread_of(edge_cells)[:2],
            pltpu.VMEM((cells_ext, LANES), jnp.int16),
            pltpu.VMEM((edges_ext, cells), BF16),
            pltpu.VMEM((edges_ext, cells), BF16),
            pltpu.VMEM(cell_edges.shape[1:], F32),
            pltpu.VMEM((edges_ext, edges), BF16),
            pltpu.VMEM((edges_ext, edges), BF16),
            pltpu.VMEM(edges_on_edge.shape[1:], F32),
            pltpu.VMEM((2 * padded, edges_ext), F32),
            pltpu.VMEM((padded, edges), F32),
            pltpu.VMEM((padded, cells), F32),
            pltpu.VMEM((padded, cells), F32),
            pltpu.VMEM((padded, cells), F32),
            pltpu.VMEM((padded, cells), F32),
            pltpu.SemaphoreType.DMA((slots,)),
            pltpu.SemaphoreType.DMA((slots,)),
            pltpu.SemaphoreType.DMA((len(arguments),)),
        ],
        compiler_params=pltpu.CompilerParams(collective_id=0, has_side_effects=True),
    )(*operands)
    results = pl.pallas_call(
        deliver,
        out_shape=tuple(jax.ShapeDtypeStruct((levels, 1, width), F32) for width in widths),
        in_specs=[vmem] * 3,
        out_specs=(hbm,) * 3,
        scratch_shapes=[pltpu.SemaphoreType.DMA((3,))],
    )(*(pltpu.with_memory_space_constraint(x, pltpu.VMEM) for x in results))
    return tuple(jnp.transpose(x, (1, 0, 2)) for x in results)


def solution(mesh):
    placed = P(("blk", "sub"), None, None)
    return jax.shard_map(
        shards,
        mesh=mesh,
        in_specs=(placed,) * 11,
        out_specs=(placed,) * 3,
        check_vma=False,
    )
```

```python
import functools

import jax
import jax.numpy as jnp
from jax import lax
from jax.experimental import pallas as pl
from jax.experimental.pallas import tpu as pltpu
from jax.sharding import PartitionSpec as P

STEP_SIZE = 0.2
OFFSETS = (1, -1, 2, -2, 3, -3)
SEND_ORDER = (4, 5, 2, 3, 0, 1, 6)
WRAP_ORDERS = {
    -1: (0, 2, 4, 5, 3, 1, 6),
    -2: (2, 4, 5, 3, 0, 1, 6),
    0: (1, 3, 5, 4, 2, 0, 6),
    1: (3, 5, 4, 2, 0, 1, 6),
    2: (5, 4, 3, 2, 0, 1, 6),
}
URGENT = 3
LANES = 128
PACKED = 16
F32 = jnp.float32
BF16 = jnp.bfloat16


def halves(values):
    lead = values.astype(BF16).astype(F32)
    return jnp.concatenate([lead, values - lead], axis=0).astype(BF16)


def dot(left, right):
    return jnp.dot(left, right, preferred_element_type=F32)


def merged_weights(indices, weights):
    total = jnp.zeros_like(weights)
    for term in range(indices.shape[0]):
        total = total + jnp.where(
            indices == indices[term : term + 1], weights[term : term + 1], 0.0
        )
    return total


def moved(indices, owned, halo, shifts):
    shift = jnp.zeros_like(indices)
    for slot, amount in enumerate(shifts):
        shift = jnp.where(indices >= owned + slot * halo, amount * halo, shift)
    return indices + shift


def build(index_ref, weight_ref, lead_ref, trail_ref, chunk, first=0, last=None):
    terms = weight_ref.shape[0]
    row_tiles = lead_ref.shape[0] // chunk
    column_tiles = lead_ref.shape[1] // LANES
    base = lax.broadcasted_iota(jnp.int32, (PACKED, LANES), 0).astype(jnp.int16)
    zero = jnp.zeros((PACKED, LANES), F32).astype(BF16)

    def tile(step, carry):
        row = pl.multiple_of(lax.rem(step, row_tiles) * chunk, chunk)
        column = pl.multiple_of(lax.div(step, row_tiles) * LANES, LANES)
        columns = pl.ds(column, LANES)

        def rows_of(ref, term):
            return jnp.broadcast_to(ref[term : term + 1, columns], (PACKED, LANES))

        indices = [(rows_of(index_ref, term) - row).astype(jnp.int16) for term in range(terms)]
        weights = [rows_of(weight_ref, term) for term in range(terms)]
        leads = [weight.astype(BF16) for weight in weights]
        if trail_ref is not None:
            trails = [
                (weight - lead.astype(F32)).astype(BF16) for weight, lead in zip(weights, leads)
            ]
        for part in range(chunk // PACKED):
            here = pl.ds(row + part * PACKED, PACKED)
            places = base + jnp.int16(part * PACKED)
            lead, trail = zero, zero
            for term in range(terms):
                hit = places == indices[term]
                lead = jnp.where(hit, leads[term], lead)
                if trail_ref is not None:
                    trail = jnp.where(hit, trails[term], trail)
            lead_ref[here, columns] = lead
            if trail_ref is not None:
                trail_ref[here, columns] = trail
        return carry

    lax.fori_loop(first, row_tiles * column_tiles if last is None else last, tile, 0)


def kernel(
    wind_hbm, density_hbm, theta_hbm, cell_edges_hbm, edge_cells_hbm, edges_on_edge_hbm,
    send_cells_hbm, send_edges_hbm, cell_weight_hbm, eoe_weight_hbm, coupling_hbm,
    tend_ref, theta_new_ref, tangential_ref,
    wind_ref, density_ref, theta_ref,
    cell_edges_ref, edge_cells_ref, edges_on_edge_ref, send_cells_ref, send_edges_ref,
    cell_weight_ref, eoe_weight_ref, coupling_ref,
    wind_ext, density_ext, theta_ext, send, received,
    average, average_weight, diverge, diverge_trail, diverge_weight,
    tangent, tangent_trail, tangent_weight,
    average_sum, tangent_sum, inverse, carried, ratios, values,
    send_sem, recv_sem, load_sem,
):
    blocks = lax.axis_size("blk")
    position = lax.axis_index("blk")
    side = lax.axis_index("sub")
    levels, edges = tangential_ref.shape
    cells = tend_ref.shape[1]
    slots, halo_cells = send_cells_ref.shape
    halo_edges = send_edges_ref.shape[1]
    padded = wind_ext.shape[0]

    def target(slot):
        if isinstance(slot, int):
            if slot == len(OFFSETS):
                return (position, 1 - side)
            return (lax.rem(position + OFFSETS[slot] + blocks, blocks), side)
        offset = (lax.div(slot, 2) + 1) * (1 - 2 * lax.rem(slot, 2))
        across = slot == len(OFFSETS)
        offset = jnp.where(across, 0, offset)
        return (lax.rem(position + offset + blocks, blocks), jnp.where(across, 1 - side, side))

    barrier = pltpu.get_barrier_semaphore()
    for slot in SEND_ORDER:
        pl.semaphore_signal(
            barrier, inc=1, device_id=target(slot), device_id_type=pl.DeviceIdType.MESH
        )

    loads = (
        (send_edges_hbm, send_edges_ref),
        (wind_hbm, wind_ref),
        (send_cells_hbm, send_cells_ref),
        (density_hbm, density_ref),
        (theta_hbm, theta_ref),
        (edge_cells_hbm, edge_cells_ref),
        (cell_edges_hbm, cell_edges_ref),
        (cell_weight_hbm, cell_weight_ref),
        (edges_on_edge_hbm, edges_on_edge_ref),
        (eoe_weight_hbm, eoe_weight_ref),
        (coupling_hbm, coupling_ref),
    )
    loads = [
        pltpu.make_async_copy(
            source.at[0] if source is edge_cells_hbm else source.at[:, 0, :], target_ref, load_sem.at[n]
        )
        for n, (source, target_ref) in enumerate(loads)
    ]
    for load in loads:
        load.start()

    for load in loads[:5]:
        load.wait()
    for ext, ref in ((wind_ext, wind_ref), (density_ext, density_ref), (theta_ext, theta_ref)):
        owned = ref.shape[1]
        ext[0:levels, 0:owned] = ref[...]
        if levels < padded:
            ext[levels:padded, 0:owned] = jnp.zeros((padded - levels, owned), F32)
    spare = cells + slots * halo_cells
    for ext in (density_ext, theta_ext):
        if spare < ext.shape[1]:
            ext[:, spare:] = jnp.zeros((padded, ext.shape[1] - spare), F32)

    upper = 2 * position >= blocks
    parity = jnp.where(upper, 1, 0)
    rank = [
        jnp.where(parity == slot % 2, 4 + slot // 2, 1 + slot // 2) for slot in range(len(OFFSETS))
    ] + [0]
    shifts = [rank[slot] - slot for slot in range(slots)]

    order = []
    for step, slot in enumerate(SEND_ORDER):
        for place, slots_there in WRAP_ORDERS.items():
            slot = jnp.where(position == lax.rem(place + blocks, blocks), slots_there[step], slot)
        order.append(slot)

    edge_rows = lax.broadcasted_iota(jnp.int32, (edges, halo_edges), 0)
    cell_rows = lax.broadcasted_iota(jnp.int32, (cells, halo_cells), 0)

    def gather(some):
        wind_own = halves(wind_ext[:, 0:edges])
        cells_own = halves(
            jnp.concatenate([density_ext[:, 0:cells], theta_ext[:, 0:cells]], axis=0)
        )
        for slot in some:
            row = pl.ds(slot, 1)
            picks = jnp.where(edge_rows == send_edges_ref[row, :], 1.0, 0.0).astype(BF16)
            both = dot(wind_own, picks)
            send[slot, :, 2 * halo_cells :] = both[0:padded] + both[padded:]
            picks = jnp.where(cell_rows == send_cells_ref[row, :], 1.0, 0.0).astype(BF16)
            both = dot(cells_own, picks)
            both = both[0 : 2 * padded] + both[2 * padded :]
            send[slot, :, 0:halo_cells] = both[0:padded]
            send[slot, :, halo_cells : 2 * halo_cells] = both[padded:]

    def copy_of(slot):
        return pltpu.make_async_remote_copy(
            src_ref=send.at[slot],
            dst_ref=received.at[slot],
            send_sem=send_sem.at[slot],
            recv_sem=recv_sem.at[slot],
            device_id=target(slot),
            device_id_type=pl.DeviceIdType.MESH,
        )

    def prepare_tangent():
        indices = moved(edges_on_edge_ref[...], edges, halo_edges, shifts)
        tangent_weight[...] = merged_weights(indices, eoe_weight_ref[...])
        edges_on_edge_ref[...] = indices

    chunk = tangent.shape[0] // 2
    tangent_steps = 2 * (tangent.shape[1] // LANES)
    tangent_ahead = jnp.where(
        position == 0, 5 * tangent_steps // 6, jnp.where(position < 3, tangent_steps // 2, 0)
    )
    early = position < 3

    gather(order[:URGENT])
    for load in loads[5:]:
        load.wait()

    @pl.when(early)
    def _():
        gather(order[URGENT:])
        prepare_tangent()
        build(edges_on_edge_ref, tangent_weight, tangent, tangent_trail, chunk, 0, tangent_ahead)

    pl.semaphore_wait(barrier, slots)
    for slot in order[:URGENT]:
        copy_of(slot).start()

    @pl.when(jnp.logical_not(early))
    def _():
        gather(order[URGENT:])

    for slot in order[URGENT:]:
        copy_of(slot).start()

    @pl.when(jnp.logical_not(early))
    def _():
        prepare_tangent()

    indices = moved(cell_edges_ref[...], edges, halo_edges, shifts)
    diverge_weight[...] = merged_weights(indices, cell_weight_ref[...])
    cell_edges_ref[...] = indices
    indices = moved(edge_cells_ref[...], cells, halo_cells, shifts)
    edge_cells_ref[:, 0:edges] = indices[:, 0:edges]
    for slot in range(slots):
        start = edges + slot * halo_edges
        place = pl.multiple_of(edges + rank[slot] * halo_edges, LANES)
        edge_cells_ref[:, pl.ds(place, halo_edges)] = indices[:, start : start + halo_edges]
    average_weight[...] = merged_weights(
        edge_cells_ref[...], jnp.full(edge_cells_ref.shape, 0.5, F32)
    )
    build(edge_cells_ref, average_weight, average, None, average.shape[0])
    build(cell_edges_ref, diverge_weight, diverge, diverge_trail, chunk)
    build(
        edges_on_edge_ref, tangent_weight, tangent, tangent_trail, chunk, tangent_ahead, tangent_steps
    )

    ratio = jnp.zeros((1, cells), F32)
    below = jnp.zeros((1, cells), F32)
    for level in range(levels):
        if level < levels - 1:
            above = coupling_ref[level : level + 1, :]
        else:
            above = jnp.zeros((1, cells), F32)
        reciprocal = 1.0 / (1.0 + below + above - below * ratio)
        ratio = above * reciprocal
        inverse[level : level + 1, :] = reciprocal
        carried[level : level + 1, :] = below * reciprocal
        ratios[level : level + 1, :] = ratio
        below = above

    def tangent_part(lower, higher):
        part = halves(wind_ext[:, lower:higher])
        both = dot(part, tangent[lower:higher, :])
        return both[0:padded] + both[padded:] + dot(
            part[0:padded], tangent_trail[lower:higher, :]
        )

    def average_part(lower, higher):
        part = density_ext[:, lower:higher]
        both = dot(
            halves(jnp.concatenate([part, part * theta_ext[:, lower:higher]], axis=0)),
            average[lower:higher, :],
        )
        return both[0 : 2 * padded] + both[2 * padded :]

    def take(slot, place):
        copy_of(slot).wait_recv()
        start = cells + place * halo_cells
        density_ext[:, start : start + halo_cells] = received[slot, :, 0:halo_cells]
        theta_ext[:, start : start + halo_cells] = received[slot, :, halo_cells : 2 * halo_cells]
        start = edges + place * halo_edges
        wind_ext[:, start : start + halo_edges] = received[slot, :, 2 * halo_cells :]

    tangent_sum[...] = tangent_part(0, edges)
    average_sum[...] = average_part(0, cells)

    near = 1 + len(OFFSETS) // 2
    take(slots - 1, 0)
    for pair in range(near - 1):
        take(2 * pair + 1 - parity, 1 + pair)
    edges_near, cells_near = edges + near * halo_edges, cells + near * halo_cells
    tangent_sum[...] += tangent_part(edges, edges_near)
    average_sum[...] += average_part(cells, cells_near)

    for pair in range(near - 1):
        take(2 * pair + parity, near + pair)
    averaged = average_sum[...] + average_part(cells_near, density_ext.shape[1])
    wind = wind_ext[...]
    fluxes = halves(jnp.concatenate([wind, wind], axis=0) * averaged)
    both = dot(fluxes, diverge[...])
    divergence = both[0 : 2 * padded] + both[2 * padded :] + dot(
        fluxes[0 : 2 * padded], diverge_trail[...]
    )
    tend_ref[...] = -divergence[0:levels]
    values[...] = (theta_ext[:, 0:cells] - STEP_SIZE * divergence[padded:])
    values[0:levels, :] = values[0:levels, :] * inverse[0:levels, :]

    tangential = tangent_sum[...] + tangent_part(edges_near, wind_ext.shape[1])
    tangential_ref[...] = tangential[0:levels]

    value = jnp.zeros((1, cells), F32)
    for level in range(levels):
        value = values[level : level + 1, :] + carried[level : level + 1, :] * value
        values[level : level + 1, :] = value
    theta_new_ref[levels - 1 : levels, :] = value
    for level in range(levels - 2, -1, -1):
        value = values[level : level + 1, :] + ratios[level : level + 1, :] * value
        theta_new_ref[level : level + 1, :] = value

    for slot in SEND_ORDER:
        copy_of(slot).wait_send()


def deliver(*refs):
    sources, targets, store_sem = refs[:3], refs[3:6], refs[6]
    stores = [
        pltpu.make_async_copy(source, target_ref.at[:, 0, :], store_sem.at[n])
        for n, (source, target_ref) in enumerate(zip(sources, targets))
    ]
    for store in stores:
        store.start()
    for store in stores:
        store.wait()


def shards(*arguments):
    wind, density, theta, cell_edges, edge_cells, edges_on_edge, send_cells, send_edges = arguments[:8]
    levels, edges = wind.shape[1:]
    cells = density.shape[2]
    slots, halo_cells = send_cells.shape[1:]
    halo_edges = send_edges.shape[2]
    padded = -(-levels // 8) * 8
    edges_ext = edge_cells.shape[2]
    cells_ext = -(-(cells + slots * halo_cells) // LANES) * LANES
    landed = [*arguments[:3], cell_edges, edge_cells, edges_on_edge, send_cells, send_edges, *arguments[8:]]
    operands = [x if x is edge_cells else jnp.transpose(x, (1, 0, 2)) for x in arguments]
    hbm = pl.BlockSpec(memory_space=pl.ANY)
    vmem = pl.BlockSpec(memory_space=pltpu.VMEM)
    widths = (cells, cells, edges)
    results = pl.pallas_call(
        kernel,
        out_shape=tuple(pltpu.VMEM((levels, width), F32) for width in widths),
        in_specs=[hbm] * len(arguments),
        out_specs=(vmem,) * 3,
        scratch_shapes=[
            *(pltpu.VMEM(x.shape[1:], x.dtype) for x in landed),
            pltpu.VMEM((padded, edges_ext), F32),
            pltpu.VMEM((padded, cells_ext), F32),
            pltpu.VMEM((padded, cells_ext), F32),
            pltpu.VMEM((slots, padded, 2 * halo_cells + halo_edges), F32),
            pltpu.VMEM((slots, padded, 2 * halo_cells + halo_edges), F32),
            pltpu.VMEM((cells_ext, edges_ext), BF16),
            pltpu.VMEM(edge_cells.shape[1:], F32),
            pltpu.VMEM((edges_ext, cells), BF16),
            pltpu.VMEM((edges_ext, cells), BF16),
            pltpu.VMEM(cell_edges.shape[1:], F32),
            pltpu.VMEM((edges_ext, edges), BF16),
            pltpu.VMEM((edges_ext, edges), BF16),
            pltpu.VMEM(edges_on_edge.shape[1:], F32),
            pltpu.VMEM((2 * padded, edges_ext), F32),
            pltpu.VMEM((padded, edges), F32),
            pltpu.VMEM((padded, cells), F32),
            pltpu.VMEM((padded, cells), F32),
            pltpu.VMEM((padded, cells), F32),
            pltpu.VMEM((padded, cells), F32),
            pltpu.SemaphoreType.DMA((slots,)),
            pltpu.SemaphoreType.DMA((slots,)),
            pltpu.SemaphoreType.DMA((len(arguments),)),
        ],
        compiler_params=pltpu.CompilerParams(collective_id=0, has_side_effects=True),
    )(*operands)
    results = pl.pallas_call(
        deliver,
        out_shape=tuple(jax.ShapeDtypeStruct((levels, 1, width), F32) for width in widths),
        in_specs=[vmem] * 3,
        out_specs=(hbm,) * 3,
        scratch_shapes=[pltpu.SemaphoreType.DMA((3,))],
    )(*(pltpu.with_memory_space_constraint(x, pltpu.VMEM) for x in results))
    return tuple(jnp.transpose(x, (1, 0, 2)) for x in results)


def solution(mesh):
    placed = P(("blk", "sub"), None, None)
    return jax.shard_map(
        shards,
        mesh=mesh,
        in_specs=(placed,) * 11,
        out_specs=(placed,) * 3,
        check_vma=False,
    )
```

```python
import functools

import jax
import jax.numpy as jnp
from jax import lax
from jax.experimental import pallas as pl
from jax.experimental.pallas import tpu as pltpu
from jax.sharding import PartitionSpec as P

STEP_SIZE = 0.2
OFFSETS = (1, -1, 2, -2, 3, -3)
SEND_ORDER = (4, 5, 2, 3, 0, 1, 6)
WRAP_ORDERS = {
    -1: (0, 2, 4, 5, 3, 1, 6),
    -2: (2, 4, 5, 3, 0, 1, 6),
    0: (4, 2, 0, 6, 1, 3, 5),
    1: (1, 4, 2, 0, 6, 3, 5),
    2: (3, 1, 4, 2, 0, 6, 5),
}
URGENT = 3
LANES = 128
PACKED = 16
F32 = jnp.float32
BF16 = jnp.bfloat16


def halves(values):
    lead = values.astype(BF16).astype(F32)
    return jnp.concatenate([lead, values - lead], axis=0).astype(BF16)


def dot(left, right):
    return jnp.dot(left, right, preferred_element_type=F32)


def merged_weights(indices, weights):
    total = jnp.zeros_like(weights)
    for term in range(indices.shape[0]):
        total = total + jnp.where(
            indices == indices[term : term + 1], weights[term : term + 1], 0.0
        )
    return total


def moved(indices, owned, halo, shifts):
    shift = jnp.zeros_like(indices)
    for slot, amount in enumerate(shifts):
        shift = jnp.where(indices >= owned + slot * halo, amount * halo, shift)
    return indices + shift


def build(index_ref, weight_ref, lead_ref, trail_ref, chunk, first=0, last=None):
    terms = weight_ref.shape[0]
    row_tiles = lead_ref.shape[0] // chunk
    column_tiles = lead_ref.shape[1] // LANES
    base = lax.broadcasted_iota(jnp.int32, (PACKED, LANES), 0).astype(jnp.int16)
    zero = jnp.zeros((PACKED, LANES), F32).astype(BF16)

    def tile(step, carry):
        row = pl.multiple_of(lax.rem(step, row_tiles) * chunk, chunk)
        column = pl.multiple_of(lax.div(step, row_tiles) * LANES, LANES)
        columns = pl.ds(column, LANES)

        def rows_of(ref, term):
            return jnp.broadcast_to(ref[term : term + 1, columns], (PACKED, LANES))

        indices = [(rows_of(index_ref, term) - row).astype(jnp.int16) for term in range(terms)]
        weights = [rows_of(weight_ref, term) for term in range(terms)]
        leads = [weight.astype(BF16) for weight in weights]
        if trail_ref is not None:
            trails = [
                (weight - lead.astype(F32)).astype(BF16) for weight, lead in zip(weights, leads)
            ]
        for part in range(chunk // PACKED):
            here = pl.ds(row + part * PACKED, PACKED)
            places = base + jnp.int16(part * PACKED)
            lead, trail = zero, zero
            for term in range(terms):
                hit = places == indices[term]
                lead = jnp.where(hit, leads[term], lead)
                if trail_ref is not None:
                    trail = jnp.where(hit, trails[term], trail)
            lead_ref[here, columns] = lead
            if trail_ref is not None:
                trail_ref[here, columns] = trail
        return carry

    lax.fori_loop(first, row_tiles * column_tiles if last is None else last, tile, 0)


def kernel(
    wind_hbm, density_hbm, theta_hbm, cell_edges_hbm, edge_cells_hbm, edges_on_edge_hbm,
    send_cells_hbm, send_edges_hbm, cell_weight_hbm, eoe_weight_hbm, coupling_hbm,
    tend_ref, theta_new_ref, tangential_ref,
    wind_ref, density_ref, theta_ref,
    cell_edges_ref, edge_cells_ref, edges_on_edge_ref, send_cells_ref, send_edges_ref,
    cell_weight_ref, eoe_weight_ref, coupling_ref,
    wind_ext, density_ext, theta_ext, send, received,
    average, average_weight, diverge, diverge_trail, diverge_weight,
    tangent, tangent_trail, tangent_weight,
    average_sum, tangent_sum, inverse, carried, ratios, values,
    send_sem, recv_sem, load_sem, near_sem, far_sem,
):
    blocks = lax.axis_size("blk")
    position = lax.axis_index("blk")
    side = lax.axis_index("sub")
    levels, edges = tangential_ref.shape
    cells = tend_ref.shape[1]
    slots, halo_cells = send_cells_ref.shape
    halo_edges = send_edges_ref.shape[1]
    padded = wind_ext.shape[0]

    def target(slot):
        if isinstance(slot, int):
            if slot == len(OFFSETS):
                return (position, 1 - side)
            return (lax.rem(position + OFFSETS[slot] + blocks, blocks), side)
        offset = (lax.div(slot, 2) + 1) * (1 - 2 * lax.rem(slot, 2))
        across = slot == len(OFFSETS)
        offset = jnp.where(across, 0, offset)
        return (lax.rem(position + offset + blocks, blocks), jnp.where(across, 1 - side, side))

    barrier = pltpu.get_barrier_semaphore()
    reach = len(OFFSETS) // 2
    first = position == 0
    waits_far = jnp.where(first, 0, jnp.maximum(reach - position, 0))
    late = jnp.where(first, reach + 1, waits_far)

    def signal(semaphore, slot):
        pl.semaphore_signal(
            semaphore, inc=1, device_id=target(slot), device_id_type=pl.DeviceIdType.MESH
        )

    def later(slot):
        if slot == len(OFFSETS):
            return first & (side == 1)
        there = position + OFFSETS[slot]
        return there > blocks if OFFSETS[slot] > 0 else there == 0

    for slot in SEND_ORDER:
        pl.when(jnp.logical_not(later(slot)))(functools.partial(signal, barrier, slot))

    loads = (
        (send_edges_hbm, send_edges_ref),
        (wind_hbm, wind_ref),
        (send_cells_hbm, send_cells_ref),
        (density_hbm, density_ref),
        (theta_hbm, theta_ref),
        (edge_cells_hbm, edge_cells_ref),
        (cell_edges_hbm, cell_edges_ref),
        (cell_weight_hbm, cell_weight_ref),
        (edges_on_edge_hbm, edges_on_edge_ref),
        (eoe_weight_hbm, eoe_weight_ref),
        (coupling_hbm, coupling_ref),
    )
    loads = [
        pltpu.make_async_copy(
            source.at[0] if source is edge_cells_hbm else source.at[:, 0, :], target_ref, load_sem.at[n]
        )
        for n, (source, target_ref) in enumerate(loads)
    ]
    for load in loads:
        load.start()

    for load in loads[:5]:
        load.wait()
    for ext, ref in ((wind_ext, wind_ref), (density_ext, density_ref), (theta_ext, theta_ref)):
        owned = ref.shape[1]
        ext[0:levels, 0:owned] = ref[...]
        if levels < padded:
            ext[levels:padded, 0:owned] = jnp.zeros((padded - levels, owned), F32)
    spare = cells + slots * halo_cells
    for ext in (density_ext, theta_ext):
        if spare < ext.shape[1]:
            ext[:, spare:] = jnp.zeros((padded, ext.shape[1] - spare), F32)

    upper = 2 * position >= blocks
    parity = jnp.where(upper, 1, 0)
    rank = [
        jnp.where(parity == slot % 2, 4 + slot // 2, 1 + slot // 2) for slot in range(len(OFFSETS))
    ] + [0]
    shifts = [rank[slot] - slot for slot in range(slots)]

    order = []
    for step, slot in enumerate(SEND_ORDER):
        for place, slots_there in WRAP_ORDERS.items():
            slot = jnp.where(position == lax.rem(place + blocks, blocks), slots_there[step], slot)
        order.append(slot)

    edge_rows = lax.broadcasted_iota(jnp.int32, (edges, halo_edges), 0)
    cell_rows = lax.broadcasted_iota(jnp.int32, (cells, halo_cells), 0)

    def gather(some):
        wind_own = halves(wind_ext[:, 0:edges])
        cells_own = halves(
            jnp.concatenate([density_ext[:, 0:cells], theta_ext[:, 0:cells]], axis=0)
        )
        for slot in some:
            row = pl.ds(slot, 1)
            picks = jnp.where(edge_rows == send_edges_ref[row, :], 1.0, 0.0).astype(BF16)
            both = dot(wind_own, picks)
            send[slot, :, 2 * halo_cells :] = both[0:padded] + both[padded:]
            picks = jnp.where(cell_rows == send_cells_ref[row, :], 1.0, 0.0).astype(BF16)
            both = dot(cells_own, picks)
            both = both[0 : 2 * padded] + both[2 * padded :]
            send[slot, :, 0:halo_cells] = both[0:padded]
            send[slot, :, halo_cells : 2 * halo_cells] = both[padded:]

    def copy_of(slot):
        return pltpu.make_async_remote_copy(
            src_ref=send.at[slot],
            dst_ref=received.at[slot],
            send_sem=send_sem.at[slot],
            recv_sem=recv_sem.at[slot],
            device_id=target(slot),
            device_id_type=pl.DeviceIdType.MESH,
        )

    chunk = tangent.shape[0] // 2
    steps = 2 * (tangent.shape[1] // LANES)
    steps_ahead = jnp.where(first, jnp.where(side == 0, 3 * steps // 4, steps // 2), 0)

    def prepare():
        indices = moved(edges_on_edge_ref[...], edges, halo_edges, shifts)
        tangent_weight[...] = merged_weights(indices, eoe_weight_ref[...])
        edges_on_edge_ref[...] = indices
        indices = moved(cell_edges_ref[...], edges, halo_edges, shifts)
        diverge_weight[...] = merged_weights(indices, cell_weight_ref[...])
        cell_edges_ref[...] = indices
        indices = moved(edge_cells_ref[...], cells, halo_cells, shifts)
        edge_cells_ref[:, 0:edges] = indices[:, 0:edges]
        for slot in range(slots):
            start = edges + slot * halo_edges
            place = pl.multiple_of(edges + rank[slot] * halo_edges, LANES)
            edge_cells_ref[:, pl.ds(place, halo_edges)] = indices[:, start : start + halo_edges]
        average_weight[...] = merged_weights(
            edge_cells_ref[...], jnp.full(edge_cells_ref.shape, 0.5, F32)
        )
        build(edge_cells_ref, average_weight, average, None, average.shape[0])
        build(cell_edges_ref, diverge_weight, diverge, diverge_trail, chunk)

    def build_tangent(lower, higher):
        build(edges_on_edge_ref, tangent_weight, tangent, tangent_trail, chunk, lower, higher)

    gather(order[:URGENT])
    for load in loads[5:]:
        load.wait()

    @pl.when(first)
    def _():
        prepare()
        build_tangent(0, steps_ahead)

    @pl.when(first)
    def _():
        pl.semaphore_wait(near_sem, reach)

    @pl.when(jnp.logical_not(first))
    def _():
        pl.semaphore_wait(barrier, slots - waits_far)
        for slot, offset in enumerate(OFFSETS):
            greeted = far_sem if offset > 0 else near_sem
            pl.when(later(slot))(functools.partial(signal, greeted, slot))

    for slot in order[:URGENT]:
        copy_of(slot).start()
    gather(order[URGENT:])
    for step, slot in enumerate(order[URGENT:], URGENT):
        pl.when(step < slots - late)(copy_of(slot).start)

    pl.when(jnp.logical_not(first))(prepare)
    build_tangent(steps_ahead, steps)

    @pl.when(first)
    def _():
        pl.semaphore_wait(barrier, reach + side)
        pl.when(side == 1)(functools.partial(signal, far_sem, slots - 1))

    greetings = jnp.where(first, 1 - side, waits_far)

    @pl.when(greetings > 0)
    def _():
        pl.semaphore_wait(far_sem, greetings)

    for step, slot in enumerate(order[URGENT:], URGENT):
        pl.when(step >= slots - late)(copy_of(slot).start)

    ratio = jnp.zeros((1, cells), F32)
    below = jnp.zeros((1, cells), F32)
    for level in range(levels):
        if level < levels - 1:
            above = coupling_ref[level : level + 1, :]
        else:
            above = jnp.zeros((1, cells), F32)
        reciprocal = 1.0 / (1.0 + below + above - below * ratio)
        ratio = above * reciprocal
        inverse[level : level + 1, :] = reciprocal
        carried[level : level + 1, :] = below * reciprocal
        ratios[level : level + 1, :] = ratio
        below = above

    def tangent_part(lower, higher):
        part = halves(wind_ext[:, lower:higher])
        both = dot(part, tangent[lower:higher, :])
        return both[0:padded] + both[padded:] + dot(
            part[0:padded], tangent_trail[lower:higher, :]
        )

    def average_part(lower, higher):
        part = density_ext[:, lower:higher]
        both = dot(
            halves(jnp.concatenate([part, part * theta_ext[:, lower:higher]], axis=0)),
            average[lower:higher, :],
        )
        return both[0 : 2 * padded] + both[2 * padded :]

    def take(slot, place):
        copy_of(slot).wait_recv()
        start = cells + place * halo_cells
        density_ext[:, start : start + halo_cells] = received[slot, :, 0:halo_cells]
        theta_ext[:, start : start + halo_cells] = received[slot, :, halo_cells : 2 * halo_cells]
        start = edges + place * halo_edges
        wind_ext[:, start : start + halo_edges] = received[slot, :, 2 * halo_cells :]

    tangent_sum[...] = tangent_part(0, edges)
    average_sum[...] = average_part(0, cells)

    near = 1 + reach
    take(slots - 1, 0)
    for pair in range(near - 1):
        take(2 * pair + 1 - parity, 1 + pair)
    edges_near, cells_near = edges + near * halo_edges, cells + near * halo_cells
    tangent_sum[...] += tangent_part(edges, edges_near)
    average_sum[...] += average_part(cells, cells_near)

    for pair in range(near - 1):
        take(2 * pair + parity, near + pair)
    averaged = average_sum[...] + average_part(cells_near, density_ext.shape[1])
    wind = wind_ext[...]
    fluxes = halves(jnp.concatenate([wind, wind], axis=0) * averaged)
    both = dot(fluxes, diverge[...])
    divergence = both[0 : 2 * padded] + both[2 * padded :] + dot(
        fluxes[0 : 2 * padded], diverge_trail[...]
    )
    tend_ref[...] = -divergence[0:levels]
    values[...] = (theta_ext[:, 0:cells] - STEP_SIZE * divergence[padded:])
    values[0:levels, :] = values[0:levels, :] * inverse[0:levels, :]

    tangential = tangent_sum[...] + tangent_part(edges_near, wind_ext.shape[1])
    tangential_ref[...] = tangential[0:levels]

    value = jnp.zeros((1, cells), F32)
    for level in range(levels):
        value = values[level : level + 1, :] + carried[level : level + 1, :] * value
        values[level : level + 1, :] = value
    theta_new_ref[levels - 1 : levels, :] = value
    for level in range(levels - 2, -1, -1):
        value = values[level : level + 1, :] + ratios[level : level + 1, :] * value
        theta_new_ref[level : level + 1, :] = value

    for slot in SEND_ORDER:
        copy_of(slot).wait_send()


def deliver(*refs):
    sources, targets, store_sem = refs[:3], refs[3:6], refs[6]
    stores = [
        pltpu.make_async_copy(source, target_ref.at[:, 0, :], store_sem.at[n])
        for n, (source, target_ref) in enumerate(zip(sources, targets))
    ]
    for store in stores:
        store.start()
    for store in stores:
        store.wait()


def shards(*arguments):
    wind, density, theta, cell_edges, edge_cells, edges_on_edge, send_cells, send_edges = arguments[:8]
    levels, edges = wind.shape[1:]
    cells = density.shape[2]
    slots, halo_cells = send_cells.shape[1:]
    halo_edges = send_edges.shape[2]
    padded = -(-levels // 8) * 8
    edges_ext = edge_cells.shape[2]
    cells_ext = -(-(cells + slots * halo_cells) // LANES) * LANES
    landed = [*arguments[:3], cell_edges, edge_cells, edges_on_edge, send_cells, send_edges, *arguments[8:]]
    operands = [x if x is edge_cells else jnp.transpose(x, (1, 0, 2)) for x in arguments]
    hbm = pl.BlockSpec(memory_space=pl.ANY)
    vmem = pl.BlockSpec(memory_space=pltpu.VMEM)
    widths = (cells, cells, edges)
    results = pl.pallas_call(
        kernel,
        out_shape=tuple(pltpu.VMEM((levels, width), F32) for width in widths),
        in_specs=[hbm] * len(arguments),
        out_specs=(vmem,) * 3,
        scratch_shapes=[
            *(pltpu.VMEM(x.shape[1:], x.dtype) for x in landed),
            pltpu.VMEM((padded, edges_ext), F32),
            pltpu.VMEM((padded, cells_ext), F32),
            pltpu.VMEM((padded, cells_ext), F32),
            pltpu.VMEM((slots, padded, 2 * halo_cells + halo_edges), F32),
            pltpu.VMEM((slots, padded, 2 * halo_cells + halo_edges), F32),
            pltpu.VMEM((cells_ext, edges_ext), BF16),
            pltpu.VMEM(edge_cells.shape[1:], F32),
            pltpu.VMEM((edges_ext, cells), BF16),
            pltpu.VMEM((edges_ext, cells), BF16),
            pltpu.VMEM(cell_edges.shape[1:], F32),
            pltpu.VMEM((edges_ext, edges), BF16),
            pltpu.VMEM((edges_ext, edges), BF16),
            pltpu.VMEM(edges_on_edge.shape[1:], F32),
            pltpu.VMEM((2 * padded, edges_ext), F32),
            pltpu.VMEM((padded, edges), F32),
            pltpu.VMEM((padded, cells), F32),
            pltpu.VMEM((padded, cells), F32),
            pltpu.VMEM((padded, cells), F32),
            pltpu.VMEM((padded, cells), F32),
            pltpu.SemaphoreType.DMA((slots,)),
            pltpu.SemaphoreType.DMA((slots,)),
            pltpu.SemaphoreType.DMA((len(arguments),)),
            pltpu.SemaphoreType.REGULAR,
            pltpu.SemaphoreType.REGULAR,
        ],
        compiler_params=pltpu.CompilerParams(collective_id=0, has_side_effects=True),
    )(*operands)
    results = pl.pallas_call(
        deliver,
        out_shape=tuple(jax.ShapeDtypeStruct((levels, 1, width), F32) for width in widths),
        in_specs=[vmem] * 3,
        out_specs=(hbm,) * 3,
        scratch_shapes=[pltpu.SemaphoreType.DMA((3,))],
    )(*(pltpu.with_memory_space_constraint(x, pltpu.VMEM) for x in results))
    return tuple(jnp.transpose(x, (1, 0, 2)) for x in results)


def solution(mesh):
    placed = P(("blk", "sub"), None, None)
    return jax.shard_map(
        shards,
        mesh=mesh,
        in_specs=(placed,) * 11,
        out_specs=(placed,) * 3,
        check_vma=False,
    )
```

```python
import functools

import jax
import jax.numpy as jnp
from jax import lax
from jax.experimental import pallas as pl
from jax.experimental.pallas import tpu as pltpu
from jax.sharding import PartitionSpec as P

STEP_SIZE = 0.2
OFFSETS = (1, -1, 2, -2, 3, -3)
SEND_ORDER = (4, 5, 2, 3, 0, 1, 6)
WRAP_ORDERS = {
    -1: (0, 2, 4, 5, 3, 1, 6),
    -2: (2, 4, 5, 3, 0, 1, 6),
    0: (4, 2, 0, 6, 1, 3, 5),
    1: (1, 4, 2, 0, 6, 3, 5),
    2: (3, 1, 4, 2, 0, 6, 5),
}
LANES = 128
PACKED = 16
F32 = jnp.float32
BF16 = jnp.bfloat16


def halves(values):
    lead = values.astype(BF16).astype(F32)
    return jnp.concatenate([lead, values - lead], axis=0).astype(BF16)


def dot(left, right):
    return jnp.dot(left, right, preferred_element_type=F32)


def merged_weights(indices, weights):
    total = jnp.zeros_like(weights)
    for term in range(indices.shape[0]):
        total = total + jnp.where(
            indices == indices[term : term + 1], weights[term : term + 1], 0.0
        )
    return total


def moved(indices, owned, halo, shifts):
    shift = jnp.zeros_like(indices)
    for slot, amount in enumerate(shifts):
        shift = jnp.where(indices >= owned + slot * halo, amount * halo, shift)
    return indices + shift


def build(index_ref, weight_ref, lead_ref, trail_ref, chunk, first=0, last=None):
    terms = weight_ref.shape[0]
    row_tiles = lead_ref.shape[0] // chunk
    column_tiles = lead_ref.shape[1] // LANES
    base = lax.broadcasted_iota(jnp.int32, (PACKED, LANES), 0).astype(jnp.int16)
    zero = jnp.zeros((PACKED, LANES), F32).astype(BF16)

    def tile(step, carry):
        row = pl.multiple_of(lax.rem(step, row_tiles) * chunk, chunk)
        column = pl.multiple_of(lax.div(step, row_tiles) * LANES, LANES)
        columns = pl.ds(column, LANES)

        def rows_of(ref, term):
            return jnp.broadcast_to(ref[term : term + 1, columns], (PACKED, LANES))

        indices = [(rows_of(index_ref, term) - row).astype(jnp.int16) for term in range(terms)]
        weights = [rows_of(weight_ref, term) for term in range(terms)]
        leads = [weight.astype(BF16) for weight in weights]
        if trail_ref is not None:
            trails = [
                (weight - lead.astype(F32)).astype(BF16) for weight, lead in zip(weights, leads)
            ]
        for part in range(chunk // PACKED):
            here = pl.ds(row + part * PACKED, PACKED)
            places = base + jnp.int16(part * PACKED)
            lead, trail = zero, zero
            for term in range(terms):
                hit = places == indices[term]
                lead = jnp.where(hit, leads[term], lead)
                if trail_ref is not None:
                    trail = jnp.where(hit, trails[term], trail)
            lead_ref[here, columns] = lead
            if trail_ref is not None:
                trail_ref[here, columns] = trail
        return carry

    lax.fori_loop(first, row_tiles * column_tiles if last is None else last, tile, 0)


def kernel(
    wind_hbm, density_hbm, theta_hbm, cell_edges_hbm, edge_cells_hbm, edges_on_edge_hbm,
    send_cells_hbm, send_edges_hbm, cell_weight_hbm, eoe_weight_hbm, coupling_hbm,
    tend_ref, theta_new_ref, tangential_ref,
    wind_ref, density_ref, theta_ref,
    cell_edges_ref, edge_cells_ref, edges_on_edge_ref, send_cells_ref, send_edges_ref,
    cell_weight_ref, eoe_weight_ref, coupling_ref,
    wind_ext, density_ext, theta_ext, send, received,
    average, average_weight, diverge, diverge_trail, diverge_weight,
    tangent, tangent_trail, tangent_weight,
    average_sum, tangent_sum, inverse, carried, ratios, values,
    send_sem, recv_sem, load_sem, near_sem, far_sem,
):
    blocks = lax.axis_size("blk")
    position = lax.axis_index("blk")
    side = lax.axis_index("sub")
    levels, edges = tangential_ref.shape
    cells = tend_ref.shape[1]
    slots, halo_cells = send_cells_ref.shape
    halo_edges = send_edges_ref.shape[1]
    padded = wind_ext.shape[0]

    def target(slot):
        if isinstance(slot, int):
            if slot == len(OFFSETS):
                return (position, 1 - side)
            return (lax.rem(position + OFFSETS[slot] + blocks, blocks), side)
        offset = (lax.div(slot, 2) + 1) * (1 - 2 * lax.rem(slot, 2))
        across = slot == len(OFFSETS)
        offset = jnp.where(across, 0, offset)
        return (lax.rem(position + offset + blocks, blocks), jnp.where(across, 1 - side, side))

    loads = (
        (send_edges_hbm, send_edges_ref),
        (wind_hbm, wind_ref),
        (send_cells_hbm, send_cells_ref),
        (density_hbm, density_ref),
        (theta_hbm, theta_ref),
        (edge_cells_hbm, edge_cells_ref),
        (cell_edges_hbm, cell_edges_ref),
        (cell_weight_hbm, cell_weight_ref),
        (edges_on_edge_hbm, edges_on_edge_ref),
        (eoe_weight_hbm, eoe_weight_ref),
        (coupling_hbm, coupling_ref),
    )
    loads = [
        pltpu.make_async_copy(
            source.at[0] if source is edge_cells_hbm else source.at[:, 0, :], target_ref, load_sem.at[n]
        )
        for n, (source, target_ref) in enumerate(loads)
    ]
    for load in loads:
        load.start()

    barrier = pltpu.get_barrier_semaphore()
    reach = len(OFFSETS) // 2
    first = position == 0
    waits_far = jnp.where(first, 0, jnp.maximum(reach - position, 0))
    late = jnp.where(first, reach + 1, waits_far)

    def signal(semaphore, slot):
        pl.semaphore_signal(
            semaphore, inc=1, device_id=target(slot), device_id_type=pl.DeviceIdType.MESH
        )

    def later(slot):
        if slot == len(OFFSETS):
            return first & (side == 1)
        there = position + OFFSETS[slot]
        return there > blocks if OFFSETS[slot] > 0 else there == 0

    for slot in SEND_ORDER:
        pl.when(jnp.logical_not(later(slot)))(functools.partial(signal, barrier, slot))

    for load in loads[:5]:
        load.wait()
    for ext, ref in ((wind_ext, wind_ref), (density_ext, density_ref), (theta_ext, theta_ref)):
        owned = ref.shape[1]
        ext[0:levels, 0:owned] = ref[...]
        if levels < padded:
            ext[levels:padded, 0:owned] = jnp.zeros((padded - levels, owned), F32)
    spare = cells + slots * halo_cells
    for ext in (density_ext, theta_ext):
        if spare < ext.shape[1]:
            ext[:, spare:] = jnp.zeros((padded, ext.shape[1] - spare), F32)

    upper = position >= reach
    parity = jnp.where(upper, 1, 0)
    final = jnp.where(upper, blocks - 1 - position, position)
    final = jnp.where(final < reach, final, reach - 1)
    rank = [
        jnp.where(
            parity == slot % 2,
            1 + reach + lax.rem(slot // 2 + 2 * reach - 1 - final, reach),
            1 + slot // 2,
        )
        for slot in range(len(OFFSETS))
    ] + [0]
    shifts = [rank[slot] - slot for slot in range(slots)]

    order = []
    for step, slot in enumerate(SEND_ORDER):
        for place, slots_there in WRAP_ORDERS.items():
            slot = jnp.where(position == lax.rem(place + blocks, blocks), slots_there[step], slot)
        order.append(slot)

    edge_rows = lax.broadcasted_iota(jnp.int32, (edges, halo_edges), 0)
    cell_rows = lax.broadcasted_iota(jnp.int32, (cells, halo_cells), 0)

    def gather(some):
        wind_own = halves(wind_ext[:, 0:edges])
        cells_own = halves(
            jnp.concatenate([density_ext[:, 0:cells], theta_ext[:, 0:cells]], axis=0)
        )
        for slot in some:
            row = pl.ds(slot, 1)
            picks = jnp.where(edge_rows == send_edges_ref[row, :], 1.0, 0.0).astype(BF16)
            both = dot(wind_own, picks)
            send[slot, :, 2 * halo_cells :] = both[0:padded] + both[padded:]
            picks = jnp.where(cell_rows == send_cells_ref[row, :], 1.0, 0.0).astype(BF16)
            both = dot(cells_own, picks)
            both = both[0 : 2 * padded] + both[2 * padded :]
            send[slot, :, 0:halo_cells] = both[0:padded]
            send[slot, :, halo_cells : 2 * halo_cells] = both[padded:]

    def copy_of(slot):
        return pltpu.make_async_remote_copy(
            src_ref=send.at[slot],
            dst_ref=received.at[slot],
            send_sem=send_sem.at[slot],
            recv_sem=recv_sem.at[slot],
            device_id=target(slot),
            device_id_type=pl.DeviceIdType.MESH,
        )

    chunk = tangent.shape[0] // 2
    steps = 2 * (tangent.shape[1] // LANES)
    steps_ahead = jnp.where(first, jnp.where(side == 0, 3 * steps // 4, steps // 2), 0)
    waits = (position >= 2) & (lax.rem(position, 2) == 0) & (position < blocks - 2)
    steps_ahead = jnp.where(waits, jnp.where(side == 0, steps // 4, steps // 6), steps_ahead)
    steps_far = jnp.where(first, steps, 7 * steps // 12)

    def prepare_tangent():
        indices = moved(edges_on_edge_ref[...], edges, halo_edges, shifts)
        tangent_weight[...] = merged_weights(indices, eoe_weight_ref[...])
        edges_on_edge_ref[...] = indices

    def prepare():
        indices = moved(cell_edges_ref[...], edges, halo_edges, shifts)
        diverge_weight[...] = merged_weights(indices, cell_weight_ref[...])
        cell_edges_ref[...] = indices
        indices = moved(edge_cells_ref[...], cells, halo_cells, shifts)
        edge_cells_ref[:, 0:edges] = indices[:, 0:edges]
        for slot in range(slots):
            start = edges + slot * halo_edges
            place = pl.multiple_of(edges + rank[slot] * halo_edges, LANES)
            edge_cells_ref[:, pl.ds(place, halo_edges)] = indices[:, start : start + halo_edges]
        average_weight[...] = merged_weights(
            edge_cells_ref[...], jnp.full(edge_cells_ref.shape, 0.5, F32)
        )
        build(edge_cells_ref, average_weight, average, None, average.shape[0])
        build(cell_edges_ref, diverge_weight, diverge, diverge_trail, chunk)

    def build_tangent(lower, higher):
        build(edges_on_edge_ref, tangent_weight, tangent, tangent_trail, chunk, lower, higher)

    gather(order[:1])
    for load in loads[5:]:
        load.wait()

    pl.when(first)(prepare)

    @pl.when(steps_ahead > 0)
    def _():
        prepare_tangent()
        build_tangent(0, steps_ahead)

    @pl.when(first)
    def _():
        pl.semaphore_wait(near_sem, reach)

    @pl.when(jnp.logical_not(first))
    def _():
        pl.semaphore_wait(barrier, slots - waits_far)
        for slot, offset in enumerate(OFFSETS):
            greeted = far_sem if offset > 0 else near_sem
            pl.when(later(slot))(functools.partial(signal, greeted, slot))

    copy_of(order[0]).start()
    for begin, end in ((1, reach), (reach, slots)):
        gather(order[begin:end])
        for step in range(begin, end):
            if step < reach:
                copy_of(order[step]).start()
            else:
                pl.when(step < slots - late)(copy_of(order[step]).start)

    pl.when(jnp.logical_not(first))(prepare)
    pl.when(steps_ahead == 0)(prepare_tangent)
    build_tangent(steps_ahead, steps_far)

    @pl.when(first)
    def _():
        pl.semaphore_wait(barrier, reach + side)
        pl.when(side == 1)(functools.partial(signal, far_sem, slots - 1))

    greetings = jnp.where(first, 1 - side, waits_far)

    @pl.when(greetings > 0)
    def _():
        pl.semaphore_wait(far_sem, greetings)

    for step in range(reach, slots):
        pl.when(step >= slots - late)(copy_of(order[step]).start)

    build_tangent(steps_far, steps)

    ratio = jnp.zeros((1, cells), F32)
    below = jnp.zeros((1, cells), F32)
    for level in range(levels):
        if level < levels - 1:
            above = coupling_ref[level : level + 1, :]
        else:
            above = jnp.zeros((1, cells), F32)
        reciprocal = 1.0 / (1.0 + below + above - below * ratio)
        ratio = above * reciprocal
        inverse[level : level + 1, :] = reciprocal
        carried[level : level + 1, :] = below * reciprocal
        ratios[level : level + 1, :] = ratio
        below = above

    def tangent_part(lower, higher):
        part = halves(wind_ext[:, lower:higher])
        both = dot(part, tangent[lower:higher, :])
        return both[0:padded] + both[padded:] + dot(
            part[0:padded], tangent_trail[lower:higher, :]
        )

    def average_part(lower, higher):
        part = density_ext[:, lower:higher]
        both = dot(
            halves(jnp.concatenate([part, part * theta_ext[:, lower:higher]], axis=0)),
            average[lower:higher, :],
        )
        return both[0 : 2 * padded] + both[2 * padded :]

    def take(slot, place):
        copy_of(slot).wait_recv()
        start = cells + place * halo_cells
        density_ext[:, start : start + halo_cells] = received[slot, :, 0:halo_cells]
        theta_ext[:, start : start + halo_cells] = received[slot, :, halo_cells : 2 * halo_cells]
        start = edges + place * halo_edges
        wind_ext[:, start : start + halo_edges] = received[slot, :, 2 * halo_cells :]

    tangent_sum[...] = tangent_part(0, edges)
    average_sum[...] = average_part(0, cells)

    near = 1 + reach
    take(slots - 1, 0)
    for pair in range(near - 1):
        take(2 * pair + 1 - parity, 1 + pair)
    edges_near, cells_near = edges + near * halo_edges, cells + near * halo_cells
    tangent_sum[...] += tangent_part(edges, edges_near)
    average_sum[...] += average_part(cells, cells_near)

    def take_late(place):
        take(2 * lax.rem(final + 1 + place, reach) + parity, near + place)

    edges_late, cells_late = edges_near + 2 * halo_edges, cells_near + 2 * halo_cells
    take_late(0)
    take_late(1)
    tangent_sum[...] += tangent_part(edges_near, edges_late)
    average_sum[...] += average_part(cells_near, cells_late)

    take_late(2)
    averaged = average_sum[...] + average_part(cells_late, density_ext.shape[1])
    wind = wind_ext[...]
    fluxes = halves(jnp.concatenate([wind, wind], axis=0) * averaged)
    both = dot(fluxes, diverge[...])
    divergence = both[0 : 2 * padded] + both[2 * padded :] + dot(
        fluxes[0 : 2 * padded], diverge_trail[...]
    )
    tend_ref[...] = -divergence[0:levels]
    values[...] = (theta_ext[:, 0:cells] - STEP_SIZE * divergence[padded:])
    values[0:levels, :] = values[0:levels, :] * inverse[0:levels, :]

    tangential = tangent_sum[...] + tangent_part(edges_late, wind_ext.shape[1])
    tangential_ref[...] = tangential[0:levels]

    value = jnp.zeros((1, cells), F32)
    for level in range(levels):
        value = values[level : level + 1, :] + carried[level : level + 1, :] * value
        values[level : level + 1, :] = value
    theta_new_ref[levels - 1 : levels, :] = value
    for level in range(levels - 2, -1, -1):
        value = values[level : level + 1, :] + ratios[level : level + 1, :] * value
        theta_new_ref[level : level + 1, :] = value

    for slot in SEND_ORDER:
        copy_of(slot).wait_send()


def deliver(*refs):
    sources, targets, store_sem = refs[:3], refs[3:6], refs[6]
    stores = [
        pltpu.make_async_copy(source, target_ref.at[:, 0, :], store_sem.at[n])
        for n, (source, target_ref) in enumerate(zip(sources, targets))
    ]
    for store in stores:
        store.start()
    for store in stores:
        store.wait()


def shards(*arguments):
    wind, density, theta, cell_edges, edge_cells, edges_on_edge, send_cells, send_edges = arguments[:8]
    levels, edges = wind.shape[1:]
    cells = density.shape[2]
    slots, halo_cells = send_cells.shape[1:]
    halo_edges = send_edges.shape[2]
    padded = -(-levels // 8) * 8
    edges_ext = edge_cells.shape[2]
    cells_ext = -(-(cells + slots * halo_cells) // LANES) * LANES
    landed = [*arguments[:3], cell_edges, edge_cells, edges_on_edge, send_cells, send_edges, *arguments[8:]]
    operands = [x if x is edge_cells else jnp.transpose(x, (1, 0, 2)) for x in arguments]
    hbm = pl.BlockSpec(memory_space=pl.ANY)
    vmem = pl.BlockSpec(memory_space=pltpu.VMEM)
    widths = (cells, cells, edges)
    results = pl.pallas_call(
        kernel,
        out_shape=tuple(pltpu.VMEM((levels, width), F32) for width in widths),
        in_specs=[hbm] * len(arguments),
        out_specs=(vmem,) * 3,
        scratch_shapes=[
            *(pltpu.VMEM(x.shape[1:], x.dtype) for x in landed),
            pltpu.VMEM((padded, edges_ext), F32),
            pltpu.VMEM((padded, cells_ext), F32),
            pltpu.VMEM((padded, cells_ext), F32),
            pltpu.VMEM((slots, padded, 2 * halo_cells + halo_edges), F32),
            pltpu.VMEM((slots, padded, 2 * halo_cells + halo_edges), F32),
            pltpu.VMEM((cells_ext, edges_ext), BF16),
            pltpu.VMEM(edge_cells.shape[1:], F32),
            pltpu.VMEM((edges_ext, cells), BF16),
            pltpu.VMEM((edges_ext, cells), BF16),
            pltpu.VMEM(cell_edges.shape[1:], F32),
            pltpu.VMEM((edges_ext, edges), BF16),
            pltpu.VMEM((edges_ext, edges), BF16),
            pltpu.VMEM(edges_on_edge.shape[1:], F32),
            pltpu.VMEM((2 * padded, edges_ext), F32),
            pltpu.VMEM((padded, edges), F32),
            pltpu.VMEM((padded, cells), F32),
            pltpu.VMEM((padded, cells), F32),
            pltpu.VMEM((padded, cells), F32),
            pltpu.VMEM((padded, cells), F32),
            pltpu.SemaphoreType.DMA((slots,)),
            pltpu.SemaphoreType.DMA((slots,)),
            pltpu.SemaphoreType.DMA((len(arguments),)),
            pltpu.SemaphoreType.REGULAR,
            pltpu.SemaphoreType.REGULAR,
        ],
        compiler_params=pltpu.CompilerParams(collective_id=0, has_side_effects=True),
    )(*operands)
    results = pl.pallas_call(
        deliver,
        out_shape=tuple(jax.ShapeDtypeStruct((levels, 1, width), F32) for width in widths),
        in_specs=[vmem] * 3,
        out_specs=(hbm,) * 3,
        scratch_shapes=[pltpu.SemaphoreType.DMA((3,))],
    )(*(pltpu.with_memory_space_constraint(x, pltpu.VMEM) for x in results))
    return tuple(jnp.transpose(x, (1, 0, 2)) for x in results)


def solution(mesh):
    placed = P(("blk", "sub"), None, None)
    return jax.shard_map(
        shards,
        mesh=mesh,
        in_specs=(placed,) * 11,
        out_specs=(placed,) * 3,
        check_vma=False,
    )
```

```python
import functools

import jax
import jax.numpy as jnp
from jax import lax
from jax.experimental import pallas as pl
from jax.experimental.pallas import tpu as pltpu
from jax.sharding import PartitionSpec as P

STEP_SIZE = 0.2
OFFSETS = (1, -1, 2, -2, 3, -3)
SEND_ORDER = (4, 5, 2, 3, 0, 1, 6)
WRAP_ORDERS = {
    -1: (0, 2, 4, 5, 3, 1, 6),
    -2: (2, 4, 5, 3, 0, 1, 6),
    0: (4, 2, 0, 6, 1, 3, 5),
    1: (1, 4, 2, 0, 6, 3, 5),
    2: (3, 1, 4, 2, 0, 6, 5),
}
LANES = 128
PACKED = 16
F32 = jnp.float32
BF16 = jnp.bfloat16


def halves(values):
    lead = values.astype(BF16).astype(F32)
    return jnp.concatenate([lead, values - lead], axis=0).astype(BF16)


def dot(left, right):
    return jnp.dot(left, right, preferred_element_type=F32)


def merged_weights(indices, weights):
    total = jnp.zeros_like(weights)
    for term in range(indices.shape[0]):
        total = total + jnp.where(
            indices == indices[term : term + 1], weights[term : term + 1], 0.0
        )
    return total


def moved(indices, owned, halo, shifts):
    shift = jnp.zeros_like(indices)
    for slot, amount in enumerate(shifts):
        shift = jnp.where(indices >= owned + slot * halo, amount * halo, shift)
    return indices + shift


def build(index_ref, weight_ref, lead_ref, trail_ref, chunk, first=0, last=None):
    terms = weight_ref.shape[0]
    row_tiles = lead_ref.shape[0] // chunk
    column_tiles = lead_ref.shape[1] // LANES
    base = lax.broadcasted_iota(jnp.int32, (PACKED, LANES), 0).astype(jnp.int16)
    zero = jnp.zeros((PACKED, LANES), F32).astype(BF16)

    def tile(step, carry):
        row = pl.multiple_of(lax.rem(step, row_tiles) * chunk, chunk)
        column = pl.multiple_of(lax.div(step, row_tiles) * LANES, LANES)
        columns = pl.ds(column, LANES)

        def rows_of(ref, term):
            return jnp.broadcast_to(ref[term : term + 1, columns], (PACKED, LANES))

        indices = [(rows_of(index_ref, term) - row).astype(jnp.int16) for term in range(terms)]
        weights = [rows_of(weight_ref, term) for term in range(terms)]
        leads = [weight.astype(BF16) for weight in weights]
        if trail_ref is not None:
            trails = [
                (weight - lead.astype(F32)).astype(BF16) for weight, lead in zip(weights, leads)
            ]
        for part in range(chunk // PACKED):
            here = pl.ds(row + part * PACKED, PACKED)
            places = base + jnp.int16(part * PACKED)
            lead, trail = zero, zero
            for term in range(terms):
                hit = places == indices[term]
                lead = jnp.where(hit, leads[term], lead)
                if trail_ref is not None:
                    trail = jnp.where(hit, trails[term], trail)
            lead_ref[here, columns] = lead
            if trail_ref is not None:
                trail_ref[here, columns] = trail
        return carry

    lax.fori_loop(first, row_tiles * column_tiles if last is None else last, tile, 0)


def kernel(
    wind_hbm, density_hbm, theta_hbm, cell_edges_hbm, edge_cells_hbm, edges_on_edge_hbm,
    send_cells_hbm, send_edges_hbm, cell_weight_hbm, eoe_weight_hbm, coupling_hbm,
    tend_ref, theta_new_ref, tangential_ref,
    wind_ref, density_ref, theta_ref,
    cell_edges_ref, edge_cells_ref, edges_on_edge_ref, send_cells_ref, send_edges_ref,
    cell_weight_ref, eoe_weight_ref, coupling_ref,
    wind_ext, density_ext, theta_ext, send, received,
    average, average_weight, diverge, diverge_trail, diverge_weight,
    tangent, tangent_trail, tangent_weight,
    average_sum, tangent_sum, inverse, carried, ratios, values,
    recv_sem, load_sem, near_sem, far_sem,
):
    blocks = lax.axis_size("blk")
    position = lax.axis_index("blk")
    side = lax.axis_index("sub")
    levels, edges = tangential_ref.shape
    cells = tend_ref.shape[1]
    slots, halo_cells = send_cells_ref.shape
    halo_edges = send_edges_ref.shape[1]
    padded = wind_ext.shape[0]

    def target(slot):
        if isinstance(slot, int):
            if slot == len(OFFSETS):
                return (position, 1 - side)
            return (lax.rem(position + OFFSETS[slot] + blocks, blocks), side)
        offset = (lax.div(slot, 2) + 1) * (1 - 2 * lax.rem(slot, 2))
        across = slot == len(OFFSETS)
        offset = jnp.where(across, 0, offset)
        return (lax.rem(position + offset + blocks, blocks), jnp.where(across, 1 - side, side))

    loads = (
        (send_edges_hbm, send_edges_ref),
        (wind_hbm, wind_ref),
        (send_cells_hbm, send_cells_ref),
        (density_hbm, density_ref),
        (theta_hbm, theta_ref),
        (edge_cells_hbm, edge_cells_ref),
        (cell_edges_hbm, cell_edges_ref),
        (cell_weight_hbm, cell_weight_ref),
        (edges_on_edge_hbm, edges_on_edge_ref),
        (eoe_weight_hbm, eoe_weight_ref),
        (coupling_hbm, coupling_ref),
    )
    loads = [
        pltpu.make_async_copy(
            source.at[0] if source is edge_cells_hbm else source.at[:, 0, :], target_ref, load_sem.at[n]
        )
        for n, (source, target_ref) in enumerate(loads)
    ]
    for load in loads:
        load.start()

    barrier = pltpu.get_barrier_semaphore()
    reach = len(OFFSETS) // 2
    first = position == 0
    waits_far = jnp.where(first, 0, jnp.maximum(reach - position, 0))
    late = jnp.where(first, reach + 1, waits_far)

    def signal(semaphore, slot):
        pl.semaphore_signal(
            semaphore, inc=1, device_id=target(slot), device_id_type=pl.DeviceIdType.MESH
        )

    def later(slot):
        if slot == len(OFFSETS):
            return first & (side == 1)
        there = position + OFFSETS[slot]
        return there > blocks if OFFSETS[slot] > 0 else there == 0

    for slot in SEND_ORDER:
        pl.when(jnp.logical_not(later(slot)))(functools.partial(signal, barrier, slot))

    for load in loads[:5]:
        load.wait()
    for ext, ref in ((wind_ext, wind_ref), (density_ext, density_ref), (theta_ext, theta_ref)):
        owned = ref.shape[1]
        ext[0:levels, 0:owned] = ref[...]
        if levels < padded:
            ext[levels:padded, 0:owned] = jnp.zeros((padded - levels, owned), F32)
    spare = cells + slots * halo_cells
    for ext in (density_ext, theta_ext):
        if spare < ext.shape[1]:
            ext[:, spare:] = jnp.zeros((padded, ext.shape[1] - spare), F32)

    upper = position >= reach
    parity = jnp.where(upper, 1, 0)
    final = jnp.where(upper, blocks - 1 - position, position)
    final = jnp.where(final < reach, final, reach - 1)
    rank = [
        jnp.where(
            parity == slot % 2,
            1 + reach + lax.rem(slot // 2 + 2 * reach - 1 - final, reach),
            1 + slot // 2,
        )
        for slot in range(len(OFFSETS))
    ] + [0]
    shifts = [rank[slot] - slot for slot in range(slots)]

    order = []
    for step, slot in enumerate(SEND_ORDER):
        for place, slots_there in WRAP_ORDERS.items():
            slot = jnp.where(position == lax.rem(place + blocks, blocks), slots_there[step], slot)
        order.append(slot)

    edge_rows = lax.broadcasted_iota(jnp.int32, (edges, halo_edges), 0)
    cell_rows = lax.broadcasted_iota(jnp.int32, (cells, halo_cells), 0)

    def gather(some):
        wind_own = halves(wind_ext[:, 0:edges])
        cells_own = halves(
            jnp.concatenate([density_ext[:, 0:cells], theta_ext[:, 0:cells]], axis=0)
        )
        for slot in some:
            row = pl.ds(slot, 1)
            picks = jnp.where(edge_rows == send_edges_ref[row, :], 1.0, 0.0).astype(BF16)
            both = dot(wind_own, picks)
            send[slot, :, 2 * halo_cells :] = both[0:padded] + both[padded:]
            picks = jnp.where(cell_rows == send_cells_ref[row, :], 1.0, 0.0).astype(BF16)
            both = dot(cells_own, picks)
            both = both[0 : 2 * padded] + both[2 * padded :]
            send[slot, :, 0:halo_cells] = both[0:padded]
            send[slot, :, halo_cells : 2 * halo_cells] = both[padded:]

    def copy_of(slot):
        return pltpu.make_async_remote_copy(
            src_ref=send.at[slot],
            dst_ref=received.at[slot],
            send_sem=load_sem.at[slot],
            recv_sem=recv_sem.at[slot],
            device_id=target(slot),
            device_id_type=pl.DeviceIdType.MESH,
        )

    chunk = tangent.shape[0] // 2
    steps = 2 * (tangent.shape[1] // LANES)
    steps_ahead = jnp.where(first, jnp.where(side == 0, 3 * steps // 4, steps // 2), 0)
    waits = (position >= 2) & (lax.rem(position, 2) == 0) & (position < blocks - 2)
    steps_ahead = jnp.where(waits, jnp.where(side == 0, steps // 4, steps // 6), steps_ahead)
    steps_far = jnp.where(first, steps, 7 * steps // 12)

    def prepare_tangent():
        indices = moved(edges_on_edge_ref[...], edges, halo_edges, shifts)
        tangent_weight[...] = merged_weights(indices, eoe_weight_ref[...])
        edges_on_edge_ref[...] = indices

    def prepare():
        indices = moved(cell_edges_ref[...], edges, halo_edges, shifts)
        diverge_weight[...] = merged_weights(indices, cell_weight_ref[...])
        cell_edges_ref[...] = indices
        indices = moved(edge_cells_ref[...], cells, halo_cells, shifts)
        edge_cells_ref[:, 0:edges] = indices[:, 0:edges]
        for slot in range(slots):
            start = edges + slot * halo_edges
            place = pl.multiple_of(edges + rank[slot] * halo_edges, LANES)
            edge_cells_ref[:, pl.ds(place, halo_edges)] = indices[:, start : start + halo_edges]
        average_weight[...] = merged_weights(
            edge_cells_ref[...], jnp.full(edge_cells_ref.shape, 0.5, F32)
        )
        build(edge_cells_ref, average_weight, average, None, average.shape[0])
        build(cell_edges_ref, diverge_weight, diverge, diverge_trail, chunk)

    def build_tangent(lower, higher):
        build(edges_on_edge_ref, tangent_weight, tangent, tangent_trail, chunk, lower, higher)

    gather(order[:1])
    for load in loads[5:]:
        load.wait()

    pl.when(first)(prepare)

    @pl.when(steps_ahead > 0)
    def _():
        prepare_tangent()
        build_tangent(0, steps_ahead)

    @pl.when(first)
    def _():
        pl.semaphore_wait(near_sem, reach)

    @pl.when(jnp.logical_not(first))
    def _():
        pl.semaphore_wait(barrier, slots - waits_far)
        for slot, offset in enumerate(OFFSETS):
            greeted = far_sem if offset > 0 else near_sem
            pl.when(later(slot))(functools.partial(signal, greeted, slot))

    copy_of(order[0]).start()
    for begin, end in ((1, reach), (reach, slots)):
        gather(order[begin:end])
        for step in range(begin, end):
            if step < reach:
                copy_of(order[step]).start()
            else:
                pl.when(step < slots - late)(copy_of(order[step]).start)

    pl.when(jnp.logical_not(first))(prepare)
    pl.when(steps_ahead == 0)(prepare_tangent)
    build_tangent(steps_ahead, steps_far)

    @pl.when(first)
    def _():
        pl.semaphore_wait(barrier, reach + side)
        pl.when(side == 1)(functools.partial(signal, far_sem, slots - 1))

    greetings = jnp.where(first, 1 - side, waits_far)

    @pl.when(greetings > 0)
    def _():
        pl.semaphore_wait(far_sem, greetings)

    for step in range(reach, slots):
        pl.when(step >= slots - late)(copy_of(order[step]).start)

    build_tangent(steps_far, steps)

    middle = levels // 2
    none = jnp.zeros((1, cells), F32)

    def interface(level):
        return coupling_ref[level : level + 1, :] if 0 <= level < levels - 1 else none

    def eliminate(level, came, ratio):
        before, after = (interface(level - 1), interface(level))[:: 1 if came < 0 else -1]
        reciprocal = 1.0 / (1.0 + before + after - before * ratio)
        inverse[level : level + 1, :] = reciprocal
        carried[level : level + 1, :] = before * reciprocal
        ratio = after * reciprocal
        ratios[level : level + 1, :] = ratio
        return ratio

    upward, downward = none, none
    for step in range(max(middle, levels - 1 - middle)):
        if step < middle:
            upward = eliminate(step, -1, upward)
        if levels - 1 - step > middle:
            downward = eliminate(levels - 1 - step, 1, downward)
    before, after = interface(middle - 1), interface(middle)
    reciprocal = 1.0 / (1.0 + before * (1.0 - upward) + after * (1.0 - downward))
    inverse[middle : middle + 1, :] = reciprocal
    carried[middle : middle + 1, :] = before * reciprocal
    ratios[middle : middle + 1, :] = after * reciprocal

    def tangent_part(lower, higher):
        part = halves(wind_ext[:, lower:higher])
        both = dot(part, tangent[lower:higher, :])
        return both[0:padded] + both[padded:] + dot(
            part[0:padded], tangent_trail[lower:higher, :]
        )

    def average_part(lower, higher):
        part = density_ext[:, lower:higher]
        both = dot(
            halves(jnp.concatenate([part, part * theta_ext[:, lower:higher]], axis=0)),
            average[lower:higher, :],
        )
        return both[0 : 2 * padded] + both[2 * padded :]

    def take(slot, place):
        start = cells + place * halo_cells
        density_ext[:, start : start + halo_cells] = received[slot, :, 0:halo_cells]
        theta_ext[:, start : start + halo_cells] = received[slot, :, halo_cells : 2 * halo_cells]
        start = edges + place * halo_edges
        wind_ext[:, start : start + halo_edges] = received[slot, :, 2 * halo_cells :]

    tangent_sum[...] = tangent_part(0, edges)
    average_sum[...] = average_part(0, cells)

    near = 1 + reach
    soon = [slots - 1] + [2 * pair + 1 - parity for pair in range(reach)]
    for slot in soon:
        copy_of(slot).wait_recv()
    for place, slot in enumerate(soon):
        take(slot, place)
    edges_near, cells_near = edges + near * halo_edges, cells + near * halo_cells
    tangent_sum[...] += tangent_part(edges, edges_near)
    average_sum[...] += average_part(cells, cells_near)

    slow = [2 * lax.rem(final + 1 + place, reach) + parity for place in range(reach)]
    edges_late, cells_late = edges_near + 2 * halo_edges, cells_near + 2 * halo_cells
    for slot in slow[:2]:
        copy_of(slot).wait_recv()
    for place in range(2):
        take(slow[place], near + place)
    tangent_sum[...] += tangent_part(edges_near, edges_late)
    average_sum[...] += average_part(cells_near, cells_late)

    copy_of(slow[2]).wait_recv()
    take(slow[2], near + 2)
    averaged = average_sum[...] + average_part(cells_late, density_ext.shape[1])
    wind = wind_ext[...]
    fluxes = halves(jnp.concatenate([wind, wind], axis=0) * averaged)
    both = dot(fluxes, diverge[...])
    divergence = both[0 : 2 * padded] + both[2 * padded :] + dot(
        fluxes[0 : 2 * padded], diverge_trail[...]
    )
    tend_ref[...] = -divergence[0:levels]
    values[...] = (theta_ext[:, 0:cells] - STEP_SIZE * divergence[padded:])
    values[0:levels, :] = values[0:levels, :] * inverse[0:levels, :]

    tangential = tangent_sum[...] + tangent_part(edges_late, wind_ext.shape[1])
    tangential_ref[...] = tangential[0:levels]

    def row(ref, level):
        return ref[level : level + 1, :]

    upward, downward = none, none
    for step in range(max(middle, levels - 1 - middle)):
        if step < middle:
            upward = row(values, step) + row(carried, step) * upward
            values[step : step + 1, :] = upward
        level = levels - 1 - step
        if level > middle:
            downward = row(values, level) + row(carried, level) * downward
            values[level : level + 1, :] = downward
    upward = (
        row(values, middle) + row(carried, middle) * upward + row(ratios, middle) * downward
    )
    theta_new_ref[middle : middle + 1, :] = upward
    downward = upward
    for step in range(1, max(middle, levels - 1 - middle) + 1):
        if middle - step >= 0:
            upward = row(values, middle - step) + row(ratios, middle - step) * upward
            theta_new_ref[middle - step : middle - step + 1, :] = upward
        level = middle + step
        if level < levels:
            downward = row(values, level) + row(ratios, level) * downward
            theta_new_ref[level : level + 1, :] = downward
    for slot in SEND_ORDER:
        copy_of(slot).wait_send()


def deliver(*refs):
    sources, targets, store_sem = refs[:3], refs[3:6], refs[6]
    stores = [
        pltpu.make_async_copy(source, target_ref.at[:, 0, :], store_sem.at[n])
        for n, (source, target_ref) in enumerate(zip(sources, targets))
    ]
    for store in stores:
        store.start()
    for store in stores:
        store.wait()


def shards(*arguments):
    wind, density, theta, cell_edges, edge_cells, edges_on_edge, send_cells, send_edges = arguments[:8]
    levels, edges = wind.shape[1:]
    cells = density.shape[2]
    slots, halo_cells = send_cells.shape[1:]
    halo_edges = send_edges.shape[2]
    padded = -(-levels // 8) * 8
    edges_ext = edge_cells.shape[2]
    cells_ext = -(-(cells + slots * halo_cells) // LANES) * LANES
    landed = [*arguments[:3], cell_edges, edge_cells, edges_on_edge, send_cells, send_edges, *arguments[8:]]
    operands = [x if x is edge_cells else jnp.transpose(x, (1, 0, 2)) for x in arguments]
    hbm = pl.BlockSpec(memory_space=pl.ANY)
    vmem = pl.BlockSpec(memory_space=pltpu.VMEM)
    widths = (cells, cells, edges)
    results = pl.pallas_call(
        kernel,
        out_shape=tuple(pltpu.VMEM((levels, width), F32) for width in widths),
        in_specs=[hbm] * len(arguments),
        out_specs=(vmem,) * 3,
        scratch_shapes=[
            *(pltpu.VMEM(x.shape[1:], x.dtype) for x in landed),
            pltpu.VMEM((padded, edges_ext), F32),
            pltpu.VMEM((padded, cells_ext), F32),
            pltpu.VMEM((padded, cells_ext), F32),
            pltpu.VMEM((slots, padded, 2 * halo_cells + halo_edges), F32),
            pltpu.VMEM((slots, padded, 2 * halo_cells + halo_edges), F32),
            pltpu.VMEM((cells_ext, edges_ext), BF16),
            pltpu.VMEM(edge_cells.shape[1:], F32),
            pltpu.VMEM((edges_ext, cells), BF16),
            pltpu.VMEM((edges_ext, cells), BF16),
            pltpu.VMEM(cell_edges.shape[1:], F32),
            pltpu.VMEM((edges_ext, edges), BF16),
            pltpu.VMEM((edges_ext, edges), BF16),
            pltpu.VMEM(edges_on_edge.shape[1:], F32),
            pltpu.VMEM((2 * padded, edges_ext), F32),
            pltpu.VMEM((padded, edges), F32),
            pltpu.VMEM((padded, cells), F32),
            pltpu.VMEM((padded, cells), F32),
            pltpu.VMEM((padded, cells), F32),
            pltpu.VMEM((padded, cells), F32),
            pltpu.SemaphoreType.DMA((slots,)),
            pltpu.SemaphoreType.DMA((len(arguments),)),
            pltpu.SemaphoreType.REGULAR,
            pltpu.SemaphoreType.REGULAR,
        ],
        compiler_params=pltpu.CompilerParams(collective_id=0, has_side_effects=True),
    )(*operands)
    results = pl.pallas_call(
        deliver,
        out_shape=tuple(jax.ShapeDtypeStruct((levels, 1, width), F32) for width in widths),
        in_specs=[vmem] * 3,
        out_specs=(hbm,) * 3,
        scratch_shapes=[pltpu.SemaphoreType.DMA((3,))],
    )(*(pltpu.with_memory_space_constraint(x, pltpu.VMEM) for x in results))
    return tuple(jnp.transpose(x, (1, 0, 2)) for x in results)


def solution(mesh):
    placed = P(("blk", "sub"), None, None)
    return jax.shard_map(
        shards,
        mesh=mesh,
        in_specs=(placed,) * 11,
        out_specs=(placed,) * 3,
        check_vma=False,
    )
```

```python
import functools

import jax
import jax.numpy as jnp
from jax import lax
from jax.experimental import pallas as pl
from jax.experimental.pallas import tpu as pltpu
from jax.sharding import PartitionSpec as P

STEP_SIZE = 0.2
OFFSETS = (1, -1, 2, -2, 3, -3)
SEND_ORDER = (4, 5, 2, 3, 0, 1, 6)
WRAP_ORDERS = {
    (-1, None): (0, 2, 4, 5, 3, 1, 6),
    (-2, None): (2, 4, 5, 3, 0, 1, 6),
    (0, None): (4, 2, 0, 6, 1, 3, 5),
    (1, 0): (1, 4, 2, 0, 6, 5, 3),
    (1, 1): (1, 4, 2, 0, 6, 3, 5),
    (2, None): (3, 1, 4, 2, 0, 6, 5),
    (3, None): (5, 3, 2, 0, 4, 1, 6),
}
LANES = 128
PACKED = 16
F32 = jnp.float32
BF16 = jnp.bfloat16


def halves(values):
    lead = values.astype(BF16).astype(F32)
    return jnp.concatenate([lead, values - lead], axis=0).astype(BF16)


def dot(left, right):
    return jnp.dot(left, right, preferred_element_type=F32)


def merged_weights(indices, weights):
    total = jnp.zeros_like(weights)
    for term in range(indices.shape[0]):
        total = total + jnp.where(
            indices == indices[term : term + 1], weights[term : term + 1], 0.0
        )
    return total


def moved(indices, owned, halo, shifts):
    shift = jnp.zeros_like(indices)
    for slot, amount in enumerate(shifts):
        shift = jnp.where(indices >= owned + slot * halo, amount * halo, shift)
    return indices + shift


def build(index_ref, weight_ref, lead_ref, trail_ref, chunk, first=0, last=None):
    terms = weight_ref.shape[0]
    row_tiles = lead_ref.shape[0] // chunk
    column_tiles = lead_ref.shape[1] // LANES
    base = lax.broadcasted_iota(jnp.int32, (PACKED, LANES), 0).astype(jnp.int16)
    zero = jnp.zeros((PACKED, LANES), F32).astype(BF16)

    def tile(step, carry):
        row = pl.multiple_of(lax.rem(step, row_tiles) * chunk, chunk)
        column = pl.multiple_of(lax.div(step, row_tiles) * LANES, LANES)
        columns = pl.ds(column, LANES)

        def rows_of(ref, term):
            return jnp.broadcast_to(ref[term : term + 1, columns], (PACKED, LANES))

        indices = [(rows_of(index_ref, term) - row).astype(jnp.int16) for term in range(terms)]
        weights = [rows_of(weight_ref, term) for term in range(terms)]
        leads = [weight.astype(BF16) for weight in weights]
        if trail_ref is not None:
            trails = [
                (weight - lead.astype(F32)).astype(BF16) for weight, lead in zip(weights, leads)
            ]
        for part in range(chunk // PACKED):
            here = pl.ds(row + part * PACKED, PACKED)
            places = base + jnp.int16(part * PACKED)
            lead, trail = zero, zero
            for term in range(terms):
                hit = places == indices[term]
                lead = jnp.where(hit, leads[term], lead)
                if trail_ref is not None:
                    trail = jnp.where(hit, trails[term], trail)
            lead_ref[here, columns] = lead
            if trail_ref is not None:
                trail_ref[here, columns] = trail
        return carry

    lax.fori_loop(first, row_tiles * column_tiles if last is None else last, tile, 0)


def kernel(
    wind_hbm, density_hbm, theta_hbm, cell_edges_hbm, edge_cells_hbm, edges_on_edge_hbm,
    send_cells_hbm, send_edges_hbm, cell_weight_hbm, eoe_weight_hbm, coupling_hbm,
    tend_ref, theta_new_ref, tangential_ref,
    wind_ref, density_ref, theta_ref,
    cell_edges_ref, edge_cells_ref, edges_on_edge_ref, send_cells_ref, send_edges_ref,
    cell_weight_ref, eoe_weight_ref, coupling_ref,
    wind_ext, density_ext, theta_ext, send, received,
    average, average_weight, diverge, diverge_trail, diverge_weight,
    tangent, tangent_trail, tangent_weight,
    average_sum, tangent_sum, inverse, carried, ratios, values,
    recv_sem, load_sem, near_sem, far_sem,
):
    blocks = lax.axis_size("blk")
    position = lax.axis_index("blk")
    side = lax.axis_index("sub")
    levels, edges = tangential_ref.shape
    cells = tend_ref.shape[1]
    slots, halo_cells = send_cells_ref.shape
    halo_edges = send_edges_ref.shape[1]
    padded = wind_ext.shape[0]

    def target(slot):
        if isinstance(slot, int):
            if slot == len(OFFSETS):
                return (position, 1 - side)
            return (lax.rem(position + OFFSETS[slot] + blocks, blocks), side)
        offset = (lax.div(slot, 2) + 1) * (1 - 2 * lax.rem(slot, 2))
        across = slot == len(OFFSETS)
        offset = jnp.where(across, 0, offset)
        return (lax.rem(position + offset + blocks, blocks), jnp.where(across, 1 - side, side))

    loads = (
        (send_edges_hbm, send_edges_ref),
        (wind_hbm, wind_ref),
        (send_cells_hbm, send_cells_ref),
        (density_hbm, density_ref),
        (theta_hbm, theta_ref),
        (edge_cells_hbm, edge_cells_ref),
        (cell_edges_hbm, cell_edges_ref),
        (cell_weight_hbm, cell_weight_ref),
        (edges_on_edge_hbm, edges_on_edge_ref),
        (eoe_weight_hbm, eoe_weight_ref),
        (coupling_hbm, coupling_ref),
    )
    loads = [
        pltpu.make_async_copy(
            source.at[0] if source is edge_cells_hbm else source.at[:, 0, :], target_ref, load_sem.at[n]
        )
        for n, (source, target_ref) in enumerate(loads)
    ]
    for load in loads:
        load.start()

    barrier = pltpu.get_barrier_semaphore()
    reach = len(OFFSETS) // 2
    first = position == 0
    waits_far = jnp.where(first, 0, jnp.maximum(reach - position, 0))
    late = jnp.where(first, reach + 1, waits_far)
    holds = position == reach

    def signal(semaphore, slot):
        pl.semaphore_signal(
            semaphore, inc=1, device_id=target(slot), device_id_type=pl.DeviceIdType.MESH
        )

    def later(slot):
        if slot == len(OFFSETS):
            return first & (side == 1)
        there = position + OFFSETS[slot]
        return there > blocks if OFFSETS[slot] > 0 else there == 0

    for slot in SEND_ORDER:
        pl.when(jnp.logical_not(later(slot)))(functools.partial(signal, barrier, slot))

    for load in loads[:5]:
        load.wait()
    for ext, ref in ((wind_ext, wind_ref), (density_ext, density_ref), (theta_ext, theta_ref)):
        owned = ref.shape[1]
        ext[0:levels, 0:owned] = ref[...]
        if levels < padded:
            ext[levels:padded, 0:owned] = jnp.zeros((padded - levels, owned), F32)
    spare = cells + slots * halo_cells
    for ext in (density_ext, theta_ext):
        if spare < ext.shape[1]:
            ext[:, spare:] = jnp.zeros((padded, ext.shape[1] - spare), F32)

    upper = position >= reach
    parity = jnp.where(upper, 1, 0)
    final = jnp.where(upper, blocks - 1 - position, position)
    final = jnp.where(final < reach, final, reach - 1)
    rank = [
        jnp.where(
            parity == slot % 2,
            1 + reach + lax.rem(slot // 2 + 2 * reach - 1 - final, reach),
            1 + slot // 2,
        )
        for slot in range(len(OFFSETS))
    ] + [0]
    shifts = [rank[slot] - slot for slot in range(slots)]

    order = []
    for step, slot in enumerate(SEND_ORDER):
        for (place, way), slots_there in WRAP_ORDERS.items():
            here = position == lax.rem(place + blocks, blocks)
            if way is not None:
                here = here & (side == way)
            slot = jnp.where(here, slots_there[step], slot)
        order.append(slot)

    edge_rows = lax.broadcasted_iota(jnp.int32, (edges, halo_edges), 0)
    cell_rows = lax.broadcasted_iota(jnp.int32, (cells, halo_cells), 0)

    def gather(some):
        wind_own = halves(wind_ext[:, 0:edges])
        cells_own = halves(
            jnp.concatenate([density_ext[:, 0:cells], theta_ext[:, 0:cells]], axis=0)
        )
        for slot in some:
            row = pl.ds(slot, 1)
            picks = jnp.where(edge_rows == send_edges_ref[row, :], 1.0, 0.0).astype(BF16)
            both = dot(wind_own, picks)
            send[slot, :, 2 * halo_cells :] = both[0:padded] + both[padded:]
            picks = jnp.where(cell_rows == send_cells_ref[row, :], 1.0, 0.0).astype(BF16)
            both = dot(cells_own, picks)
            both = both[0 : 2 * padded] + both[2 * padded :]
            send[slot, :, 0:halo_cells] = both[0:padded]
            send[slot, :, halo_cells : 2 * halo_cells] = both[padded:]

    def copy_of(slot):
        return pltpu.make_async_remote_copy(
            src_ref=send.at[slot],
            dst_ref=received.at[slot],
            send_sem=load_sem.at[slot],
            recv_sem=recv_sem.at[slot],
            device_id=target(slot),
            device_id_type=pl.DeviceIdType.MESH,
        )

    chunk = tangent.shape[0] // 2
    steps = 2 * (tangent.shape[1] // LANES)
    steps_ahead = jnp.where(
        first, jnp.where(side == 0, 7 * steps // 12, steps // 4), 0
    )
    waits = (lax.rem(position, 2) == 0) & (position < blocks - 2)
    steps_far = jnp.where(first, steps, 7 * steps // 12)

    def prepare_tangent():
        indices = moved(edges_on_edge_ref[...], edges, halo_edges, shifts)
        tangent_weight[...] = merged_weights(indices, eoe_weight_ref[...])
        edges_on_edge_ref[...] = indices

    def prepare_average():
        indices = moved(edge_cells_ref[...], cells, halo_cells, shifts)
        edge_cells_ref[:, 0:edges] = indices[:, 0:edges]
        for slot in range(slots):
            start = edges + slot * halo_edges
            place = pl.multiple_of(edges + rank[slot] * halo_edges, LANES)
            edge_cells_ref[:, pl.ds(place, halo_edges)] = indices[:, start : start + halo_edges]
        average_weight[...] = merged_weights(
            edge_cells_ref[...], jnp.full(edge_cells_ref.shape, 0.5, F32)
        )
        build(edge_cells_ref, average_weight, average, None, average.shape[0])

    def prepare_diverge():
        indices = moved(cell_edges_ref[...], edges, halo_edges, shifts)
        diverge_weight[...] = merged_weights(indices, cell_weight_ref[...])
        cell_edges_ref[...] = indices
        build(cell_edges_ref, diverge_weight, diverge, diverge_trail, chunk)

    def build_tangent(lower, higher):
        build(edges_on_edge_ref, tangent_weight, tangent, tangent_trail, chunk, lower, higher)

    gather(order[:1])
    for load in loads[5:]:
        load.wait()

    pl.when(waits)(functools.partial(gather, order[1:]))
    pl.when(first)(prepare_average)
    pl.when(first)(prepare_diverge)

    @pl.when(steps_ahead > 0)
    def _():
        prepare_tangent()
        build_tangent(0, steps_ahead)

    @pl.when(first)
    def _():
        pl.semaphore_wait(near_sem, reach)

    @pl.when(jnp.logical_not(first))
    def _():
        pl.semaphore_wait(barrier, slots - waits_far)
        for slot, offset in enumerate(OFFSETS):
            greeted = far_sem if offset > 0 else near_sem
            pl.when(later(slot))(functools.partial(signal, greeted, slot))

    copy_of(order[0]).start()
    for begin, end in ((1, reach), (reach, slots)):
        pl.when(jnp.logical_not(waits))(functools.partial(gather, order[begin:end]))
        for step in range(begin, end):
            if step < reach:
                copy_of(order[step]).start()
            else:
                now = (step < slots - late) & jnp.logical_not(holds)
                pl.when(now)(copy_of(order[step]).start)

    pl.when(jnp.logical_not(first))(prepare_average)

    @pl.when(holds)
    def _():
        for slot in order[reach:]:
            copy_of(slot).start()

    pl.when(jnp.logical_not(first))(prepare_diverge)
    pl.when(steps_ahead == 0)(prepare_tangent)
    build_tangent(steps_ahead, steps_far)

    @pl.when(first)
    def _():
        pl.semaphore_wait(barrier, reach + side)
        pl.when(side == 1)(functools.partial(signal, far_sem, slots - 1))

    greetings = jnp.where(first, 1 - side, waits_far)

    @pl.when(greetings > 0)
    def _():
        pl.semaphore_wait(far_sem, greetings)

    for step in range(reach, slots):
        pl.when(step >= slots - late)(copy_of(order[step]).start)

    build_tangent(steps_far, steps)

    middle = levels // 2
    none = jnp.zeros((1, cells), F32)

    def interface(level):
        return coupling_ref[level : level + 1, :] if 0 <= level < levels - 1 else none

    def eliminate(level, came, ratio):
        before, after = (interface(level - 1), interface(level))[:: 1 if came < 0 else -1]
        reciprocal = 1.0 / (1.0 + before + after - before * ratio)
        inverse[level : level + 1, :] = reciprocal
        carried[level : level + 1, :] = before * reciprocal
        ratio = after * reciprocal
        ratios[level : level + 1, :] = ratio
        return ratio

    upward, downward = none, none
    for step in range(max(middle, levels - 1 - middle)):
        if step < middle:
            upward = eliminate(step, -1, upward)
        if levels - 1 - step > middle:
            downward = eliminate(levels - 1 - step, 1, downward)
    before, after = interface(middle - 1), interface(middle)
    reciprocal = 1.0 / (1.0 + before * (1.0 - upward) + after * (1.0 - downward))
    inverse[middle : middle + 1, :] = reciprocal
    carried[middle : middle + 1, :] = before * reciprocal
    ratios[middle : middle + 1, :] = after * reciprocal

    def tangent_part(lower, higher):
        part = halves(wind_ext[:, lower:higher])
        both = dot(part, tangent[lower:higher, :])
        return both[0:padded] + both[padded:] + dot(
            part[0:padded], tangent_trail[lower:higher, :]
        )

    def average_part(lower, higher):
        part = density_ext[:, lower:higher]
        both = dot(
            halves(jnp.concatenate([part, part * theta_ext[:, lower:higher]], axis=0)),
            average[lower:higher, :],
        )
        return both[0 : 2 * padded] + both[2 * padded :]

    def take(slot, place):
        start = cells + place * halo_cells
        density_ext[:, start : start + halo_cells] = received[slot, :, 0:halo_cells]
        theta_ext[:, start : start + halo_cells] = received[slot, :, halo_cells : 2 * halo_cells]
        start = edges + place * halo_edges
        wind_ext[:, start : start + halo_edges] = received[slot, :, 2 * halo_cells :]

    tangent_sum[...] = tangent_part(0, edges)
    average_sum[...] = average_part(0, cells)

    near = 1 + reach
    soon = [slots - 1] + [2 * pair + 1 - parity for pair in range(reach)]
    for slot in soon:
        copy_of(slot).wait_recv()
    for place, slot in enumerate(soon):
        take(slot, place)
    edges_near, cells_near = edges + near * halo_edges, cells + near * halo_cells
    tangent_sum[...] += tangent_part(edges, edges_near)
    average_sum[...] += average_part(cells, cells_near)

    slow = [2 * lax.rem(final + 1 + place, reach) + parity for place in range(reach)]
    edges_late, cells_late = edges_near + 2 * halo_edges, cells_near + 2 * halo_cells
    for slot in slow[:2]:
        copy_of(slot).wait_recv()
    for place in range(2):
        take(slow[place], near + place)
    tangent_sum[...] += tangent_part(edges_near, edges_late)
    average_sum[...] += average_part(cells_near, cells_late)

    copy_of(slow[2]).wait_recv()
    take(slow[2], near + 2)
    averaged = average_sum[...] + average_part(cells_late, density_ext.shape[1])
    wind = wind_ext[...]
    fluxes = halves(jnp.concatenate([wind, wind], axis=0) * averaged)
    both = dot(fluxes, diverge[...])
    divergence = both[0 : 2 * padded] + both[2 * padded :] + dot(
        fluxes[0 : 2 * padded], diverge_trail[...]
    )
    tend_ref[...] = -divergence[0:levels]
    values[...] = (theta_ext[:, 0:cells] - STEP_SIZE * divergence[padded:])
    values[0:levels, :] = values[0:levels, :] * inverse[0:levels, :]

    tangential = tangent_sum[...] + tangent_part(edges_late, wind_ext.shape[1])
    tangential_ref[...] = tangential[0:levels]

    def row(ref, level):
        return ref[level : level + 1, :]

    upward, downward = none, none
    for step in range(max(middle, levels - 1 - middle)):
        if step < middle:
            upward = row(values, step) + row(carried, step) * upward
            values[step : step + 1, :] = upward
        level = levels - 1 - step
        if level > middle:
            downward = row(values, level) + row(carried, level) * downward
            values[level : level + 1, :] = downward
    upward = (
        row(values, middle) + row(carried, middle) * upward + row(ratios, middle) * downward
    )
    theta_new_ref[middle : middle + 1, :] = upward
    downward = upward
    for step in range(1, max(middle, levels - 1 - middle) + 1):
        if middle - step >= 0:
            upward = row(values, middle - step) + row(ratios, middle - step) * upward
            theta_new_ref[middle - step : middle - step + 1, :] = upward
        level = middle + step
        if level < levels:
            downward = row(values, level) + row(ratios, level) * downward
            theta_new_ref[level : level + 1, :] = downward
    for slot in SEND_ORDER:
        copy_of(slot).wait_send()


def deliver(*refs):
    sources, targets, store_sem = refs[:3], refs[3:6], refs[6]
    stores = [
        pltpu.make_async_copy(source, target_ref.at[:, 0, :], store_sem.at[n])
        for n, (source, target_ref) in enumerate(zip(sources, targets))
    ]
    for store in stores:
        store.start()
    for store in stores:
        store.wait()


def shards(*arguments):
    wind, density, theta, cell_edges, edge_cells, edges_on_edge, send_cells, send_edges = arguments[:8]
    levels, edges = wind.shape[1:]
    cells = density.shape[2]
    slots, halo_cells = send_cells.shape[1:]
    halo_edges = send_edges.shape[2]
    padded = -(-levels // 8) * 8
    edges_ext = edge_cells.shape[2]
    cells_ext = -(-(cells + slots * halo_cells) // LANES) * LANES
    landed = [*arguments[:3], cell_edges, edge_cells, edges_on_edge, send_cells, send_edges, *arguments[8:]]
    operands = [x if x is edge_cells else jnp.transpose(x, (1, 0, 2)) for x in arguments]
    hbm = pl.BlockSpec(memory_space=pl.ANY)
    vmem = pl.BlockSpec(memory_space=pltpu.VMEM)
    widths = (cells, cells, edges)
    results = pl.pallas_call(
        kernel,
        out_shape=tuple(pltpu.VMEM((levels, width), F32) for width in widths),
        in_specs=[hbm] * len(arguments),
        out_specs=(vmem,) * 3,
        scratch_shapes=[
            *(pltpu.VMEM(x.shape[1:], x.dtype) for x in landed),
            pltpu.VMEM((padded, edges_ext), F32),
            pltpu.VMEM((padded, cells_ext), F32),
            pltpu.VMEM((padded, cells_ext), F32),
            pltpu.VMEM((slots, padded, 2 * halo_cells + halo_edges), F32),
            pltpu.VMEM((slots, padded, 2 * halo_cells + halo_edges), F32),
            pltpu.VMEM((cells_ext, edges_ext), BF16),
            pltpu.VMEM(edge_cells.shape[1:], F32),
            pltpu.VMEM((edges_ext, cells), BF16),
            pltpu.VMEM((edges_ext, cells), BF16),
            pltpu.VMEM(cell_edges.shape[1:], F32),
            pltpu.VMEM((edges_ext, edges), BF16),
            pltpu.VMEM((edges_ext, edges), BF16),
            pltpu.VMEM(edges_on_edge.shape[1:], F32),
            pltpu.VMEM((2 * padded, edges_ext), F32),
            pltpu.VMEM((padded, edges), F32),
            pltpu.VMEM((padded, cells), F32),
            pltpu.VMEM((padded, cells), F32),
            pltpu.VMEM((padded, cells), F32),
            pltpu.VMEM((padded, cells), F32),
            pltpu.SemaphoreType.DMA((slots,)),
            pltpu.SemaphoreType.DMA((len(arguments),)),
            pltpu.SemaphoreType.REGULAR,
            pltpu.SemaphoreType.REGULAR,
        ],
        compiler_params=pltpu.CompilerParams(collective_id=0, has_side_effects=True),
    )(*operands)
    results = pl.pallas_call(
        deliver,
        out_shape=tuple(jax.ShapeDtypeStruct((levels, 1, width), F32) for width in widths),
        in_specs=[vmem] * 3,
        out_specs=(hbm,) * 3,
        scratch_shapes=[pltpu.SemaphoreType.DMA((3,))],
    )(*(pltpu.with_memory_space_constraint(x, pltpu.VMEM) for x in results))
    return tuple(jnp.transpose(x, (1, 0, 2)) for x in results)


def solution(mesh):
    placed = P(("blk", "sub"), None, None)
    return jax.shard_map(
        shards,
        mesh=mesh,
        in_specs=(placed,) * 11,
        out_specs=(placed,) * 3,
        check_vma=False,
    )
```

```python
import functools

import jax
import jax.numpy as jnp
from jax import lax
from jax.experimental import pallas as pl
from jax.experimental.pallas import tpu as pltpu
from jax.sharding import PartitionSpec as P

STEP_SIZE = 0.2
OFFSETS = (1, -1, 2, -2, 3, -3)
SEND_ORDER = (4, 5, 2, 3, 0, 1, 6)
WRAP_ORDERS = {
    (-1, None): (0, 2, 4, 5, 3, 1, 6),
    (-2, None): (2, 4, 5, 3, 0, 1, 6),
    (0, None): (4, 2, 0, 6, 1, 3, 5),
    (1, 0): (1, 4, 2, 0, 6, 5, 3),
    (1, 1): (1, 4, 2, 0, 6, 3, 5),
    (2, None): (3, 1, 4, 2, 0, 6, 5),
    (3, None): (5, 3, 2, 0, 4, 1, 6),
}
LANES = 128
PACKED = 16
F32 = jnp.float32
BF16 = jnp.bfloat16


def halves(values):
    lead = values.astype(BF16).astype(F32)
    return jnp.concatenate([lead, values - lead], axis=0).astype(BF16)


def dot(left, right):
    return jnp.dot(left, right, preferred_element_type=F32)


def merged_weights(indices, weights):
    total = jnp.zeros_like(weights)
    for term in range(indices.shape[0]):
        total = total + jnp.where(
            indices == indices[term : term + 1], weights[term : term + 1], 0.0
        )
    return total


def moved(indices, owned, halo, shifts):
    shift = jnp.zeros_like(indices)
    for slot, amount in enumerate(shifts):
        shift = jnp.where(indices >= owned + slot * halo, amount * halo, shift)
    return indices + shift


def build(index_ref, weight_ref, lead_ref, trail_ref, chunk, first=0, last=None):
    terms = weight_ref.shape[0]
    row_tiles = lead_ref.shape[0] // chunk
    column_tiles = lead_ref.shape[1] // LANES
    base = lax.broadcasted_iota(jnp.int32, (PACKED, LANES), 0).astype(jnp.int16)
    zero = jnp.zeros((PACKED, LANES), F32).astype(BF16)

    def tile(step, carry):
        row = pl.multiple_of(lax.rem(step, row_tiles) * chunk, chunk)
        column = pl.multiple_of(lax.div(step, row_tiles) * LANES, LANES)
        columns = pl.ds(column, LANES)

        def rows_of(ref, term):
            return jnp.broadcast_to(ref[term : term + 1, columns], (PACKED, LANES))

        indices = [(rows_of(index_ref, term) - row).astype(jnp.int16) for term in range(terms)]
        weights = [rows_of(weight_ref, term) for term in range(terms)]
        leads = [weight.astype(BF16) for weight in weights]
        if trail_ref is not None:
            trails = [
                (weight - lead.astype(F32)).astype(BF16) for weight, lead in zip(weights, leads)
            ]
        for part in range(chunk // PACKED):
            here = pl.ds(row + part * PACKED, PACKED)
            places = base + jnp.int16(part * PACKED)
            lead, trail = zero, zero
            for term in range(terms):
                hit = places == indices[term]
                lead = jnp.where(hit, leads[term], lead)
                if trail_ref is not None:
                    trail = jnp.where(hit, trails[term], trail)
            lead_ref[here, columns] = lead
            if trail_ref is not None:
                trail_ref[here, columns] = trail
        return carry

    lax.fori_loop(first, row_tiles * column_tiles if last is None else last, tile, 0)


def kernel(
    wind_hbm, density_hbm, theta_hbm, cell_edges_hbm, edge_cells_hbm, edges_on_edge_hbm,
    send_cells_hbm, send_edges_hbm, cell_weight_hbm, eoe_weight_hbm, coupling_hbm,
    tend_ref, theta_new_ref, tangential_ref,
    wind_ref, density_ref, theta_ref,
    cell_edges_ref, edge_cells_ref, edges_on_edge_ref, send_cells_ref, send_edges_ref,
    cell_weight_ref, eoe_weight_ref, coupling_ref,
    wind_ext, density_ext, theta_ext, send, received,
    average, average_weight, diverge, diverge_trail, diverge_weight,
    tangent, tangent_trail, tangent_weight,
    average_sum, tangent_sum, inverse, carried, ratios, values,
    recv_sem, load_sem, near_sem, far_sem,
):
    blocks = lax.axis_size("blk")
    position = lax.axis_index("blk")
    side = lax.axis_index("sub")
    levels, edges = tangential_ref.shape
    cells = tend_ref.shape[1]
    slots, halo_cells = send_cells_ref.shape
    halo_edges = send_edges_ref.shape[1]
    padded = wind_ext.shape[0]

    def target(slot):
        if isinstance(slot, int):
            if slot == len(OFFSETS):
                return (position, 1 - side)
            return (lax.rem(position + OFFSETS[slot] + blocks, blocks), side)
        offset = (lax.div(slot, 2) + 1) * (1 - 2 * lax.rem(slot, 2))
        across = slot == len(OFFSETS)
        offset = jnp.where(across, 0, offset)
        return (lax.rem(position + offset + blocks, blocks), jnp.where(across, 1 - side, side))

    loads = (
        (send_edges_hbm, send_edges_ref),
        (send_cells_hbm, send_cells_ref),
        (wind_hbm, wind_ref),
        (density_hbm, density_ref),
        (theta_hbm, theta_ref),
        (edge_cells_hbm, edge_cells_ref),
        (cell_edges_hbm, cell_edges_ref),
        (cell_weight_hbm, cell_weight_ref),
        (edges_on_edge_hbm, edges_on_edge_ref),
        (eoe_weight_hbm, eoe_weight_ref),
        (coupling_hbm, coupling_ref),
    )
    loads = [
        pltpu.make_async_copy(
            source.at[0] if source is edge_cells_hbm else source.at[:, 0, :], target_ref, load_sem.at[n]
        )
        for n, (source, target_ref) in enumerate(loads)
    ]
    for load in loads:
        load.start()

    barrier = pltpu.get_barrier_semaphore()
    reach = len(OFFSETS) // 2
    first = position == 0
    waits_far = jnp.where(first, 0, jnp.maximum(reach - position, 0))
    late = jnp.where(first, reach + 1, waits_far)
    holds = position == reach

    def signal(semaphore, slot):
        pl.semaphore_signal(
            semaphore, inc=1, device_id=target(slot), device_id_type=pl.DeviceIdType.MESH
        )

    def later(slot):
        if slot == len(OFFSETS):
            return first & (side == 1)
        there = position + OFFSETS[slot]
        return there > blocks if OFFSETS[slot] > 0 else there == 0

    for slot in SEND_ORDER:
        pl.when(jnp.logical_not(later(slot)))(functools.partial(signal, barrier, slot))

    def keep(ext, ref):
        owned = ref.shape[1]
        ext[0:levels, 0:owned] = ref[...]
        if levels < padded:
            ext[levels:padded, 0:owned] = jnp.zeros((padded - levels, owned), F32)

    upper = position >= reach
    parity = jnp.where(upper, 1, 0)
    final = jnp.where(upper, blocks - 1 - position, position)
    final = jnp.where(final < reach, final, reach - 1)
    rank = [
        jnp.where(
            parity == slot % 2,
            1 + reach + lax.rem(slot // 2 + 2 * reach - 1 - final, reach),
            1 + slot // 2,
        )
        for slot in range(len(OFFSETS))
    ] + [0]
    shifts = [rank[slot] - slot for slot in range(slots)]

    order = []
    for step, slot in enumerate(SEND_ORDER):
        for (place, way), slots_there in WRAP_ORDERS.items():
            here = position == lax.rem(place + blocks, blocks)
            if way is not None:
                here = here & (side == way)
            slot = jnp.where(here, slots_there[step], slot)
        order.append(slot)

    edge_rows = lax.broadcasted_iota(jnp.int32, (edges, halo_edges), 0)
    cell_rows = lax.broadcasted_iota(jnp.int32, (cells, halo_cells), 0)

    def edge_picks(slot):
        return jnp.where(edge_rows == send_edges_ref[pl.ds(slot, 1), :], 1.0, 0.0).astype(BF16)

    def cell_picks(slot):
        return jnp.where(cell_rows == send_cells_ref[pl.ds(slot, 1), :], 1.0, 0.0).astype(BF16)

    def own_wind():
        return halves(wind_ext[:, 0:edges])

    def own_cells():
        return halves(
            jnp.concatenate([density_ext[:, 0:cells], theta_ext[:, 0:cells]], axis=0)
        )

    def pack_wind(slot, both):
        send[slot, :, 2 * halo_cells :] = both[0:padded] + both[padded:]

    def pack_cells(slot, both):
        both = both[0 : 2 * padded] + both[2 * padded :]
        send[slot, :, 0:halo_cells] = both[0:padded]
        send[slot, :, halo_cells : 2 * halo_cells] = both[padded:]

    def gather(some):
        wind_own, cells_own = own_wind(), own_cells()
        for slot in some:
            pack_wind(slot, dot(wind_own, edge_picks(slot)))
            pack_cells(slot, dot(cells_own, cell_picks(slot)))

    def copy_of(slot):
        return pltpu.make_async_remote_copy(
            src_ref=send.at[slot],
            dst_ref=received.at[slot],
            send_sem=load_sem.at[slot],
            recv_sem=recv_sem.at[slot],
            device_id=target(slot),
            device_id_type=pl.DeviceIdType.MESH,
        )

    chunk = tangent.shape[0] // 2
    steps = 2 * (tangent.shape[1] // LANES)
    steps_ahead = jnp.where(
        first, jnp.where(side == 0, 7 * steps // 12, steps // 4), 0
    )
    waits = (lax.rem(position, 2) == 0) & (position < blocks - 2)
    steps_far = jnp.where(first, steps, 7 * steps // 12)

    def prepare_tangent():
        indices = moved(edges_on_edge_ref[...], edges, halo_edges, shifts)
        tangent_weight[...] = merged_weights(indices, eoe_weight_ref[...])
        edges_on_edge_ref[...] = indices

    def prepare_average():
        indices = moved(edge_cells_ref[...], cells, halo_cells, shifts)
        edge_cells_ref[:, 0:edges] = indices[:, 0:edges]
        for slot in range(slots):
            start = edges + slot * halo_edges
            place = pl.multiple_of(edges + rank[slot] * halo_edges, LANES)
            edge_cells_ref[:, pl.ds(place, halo_edges)] = indices[:, start : start + halo_edges]
        average_weight[...] = merged_weights(
            edge_cells_ref[...], jnp.full(edge_cells_ref.shape, 0.5, F32)
        )
        build(edge_cells_ref, average_weight, average, None, average.shape[0])

    def prepare_diverge():
        indices = moved(cell_edges_ref[...], edges, halo_edges, shifts)
        diverge_weight[...] = merged_weights(indices, cell_weight_ref[...])
        cell_edges_ref[...] = indices
        build(cell_edges_ref, diverge_weight, diverge, diverge_trail, chunk)

    def build_tangent(lower, higher):
        build(edges_on_edge_ref, tangent_weight, tangent, tangent_trail, chunk, lower, higher)

    for load in loads[:2]:
        load.wait()
    picks = edge_picks(order[0]), cell_picks(order[0])
    for load in loads[2:5]:
        load.wait()
    keep(wind_ext, wind_ref)
    keep(density_ext, density_ref)
    keep(theta_ext, theta_ref)
    pack_wind(order[0], dot(own_wind(), picks[0]))
    pack_cells(order[0], dot(own_cells(), picks[1]))
    spare = cells + slots * halo_cells
    for ext in (density_ext, theta_ext):
        if spare < ext.shape[1]:
            ext[:, spare:] = jnp.zeros((padded, ext.shape[1] - spare), F32)
    for load in loads[5:]:
        load.wait()

    pl.when(waits)(functools.partial(gather, order[1:]))
    pl.when(first)(prepare_average)
    pl.when(first)(prepare_diverge)

    @pl.when(steps_ahead > 0)
    def _():
        prepare_tangent()
        build_tangent(0, steps_ahead)

    @pl.when(first)
    def _():
        pl.semaphore_wait(near_sem, reach)

    @pl.when(jnp.logical_not(first))
    def _():
        pl.semaphore_wait(barrier, slots - waits_far)
        for slot, offset in enumerate(OFFSETS):
            greeted = far_sem if offset > 0 else near_sem
            pl.when(later(slot))(functools.partial(signal, greeted, slot))

    copy_of(order[0]).start()
    for begin, end in ((1, reach), (reach, slots)):
        pl.when(jnp.logical_not(waits))(functools.partial(gather, order[begin:end]))
        for step in range(begin, end):
            if step < reach:
                copy_of(order[step]).start()
            else:
                now = (step < slots - late) & jnp.logical_not(holds)
                pl.when(now)(copy_of(order[step]).start)

    pl.when(jnp.logical_not(first))(prepare_average)

    @pl.when(holds)
    def _():
        for slot in order[reach:]:
            copy_of(slot).start()

    pl.when(jnp.logical_not(first))(prepare_diverge)
    pl.when(steps_ahead == 0)(prepare_tangent)
    build_tangent(steps_ahead, steps_far)

    @pl.when(first)
    def _():
        pl.semaphore_wait(barrier, reach + side)
        pl.when(side == 1)(functools.partial(signal, far_sem, slots - 1))

    greetings = jnp.where(first, 1 - side, waits_far)

    @pl.when(greetings > 0)
    def _():
        pl.semaphore_wait(far_sem, greetings)

    for step in range(reach, slots):
        pl.when(step >= slots - late)(copy_of(order[step]).start)

    build_tangent(steps_far, steps)

    middle = levels // 2
    none = jnp.zeros((1, cells), F32)

    def interface(level):
        return coupling_ref[level : level + 1, :] if 0 <= level < levels - 1 else none

    def eliminate(level, came, ratio):
        before, after = (interface(level - 1), interface(level))[:: 1 if came < 0 else -1]
        reciprocal = 1.0 / (1.0 + before + after - before * ratio)
        inverse[level : level + 1, :] = reciprocal
        carried[level : level + 1, :] = before * reciprocal
        ratio = after * reciprocal
        ratios[level : level + 1, :] = ratio
        return ratio

    upward, downward = none, none
    for step in range(max(middle, levels - 1 - middle)):
        if step < middle:
            upward = eliminate(step, -1, upward)
        if levels - 1 - step > middle:
            downward = eliminate(levels - 1 - step, 1, downward)
    before, after = interface(middle - 1), interface(middle)
    reciprocal = 1.0 / (1.0 + before * (1.0 - upward) + after * (1.0 - downward))
    inverse[middle : middle + 1, :] = reciprocal
    carried[middle : middle + 1, :] = before * reciprocal
    ratios[middle : middle + 1, :] = after * reciprocal

    def tangent_part(lower, higher):
        part = halves(wind_ext[:, lower:higher])
        both = dot(part, tangent[lower:higher, :])
        return both[0:padded] + both[padded:] + dot(
            part[0:padded], tangent_trail[lower:higher, :]
        )

    def average_part(lower, higher):
        part = density_ext[:, lower:higher]
        both = dot(
            halves(jnp.concatenate([part, part * theta_ext[:, lower:higher]], axis=0)),
            average[lower:higher, :],
        )
        return both[0 : 2 * padded] + both[2 * padded :]

    def take(slot, place):
        start = cells + place * halo_cells
        density_ext[:, start : start + halo_cells] = received[slot, :, 0:halo_cells]
        theta_ext[:, start : start + halo_cells] = received[slot, :, halo_cells : 2 * halo_cells]
        start = edges + place * halo_edges
        wind_ext[:, start : start + halo_edges] = received[slot, :, 2 * halo_cells :]

    tangent_sum[...] = tangent_part(0, edges)
    average_sum[...] = average_part(0, cells)

    near = 1 + reach
    soon = [slots - 1] + [2 * pair + 1 - parity for pair in range(reach)]
    for slot in soon:
        copy_of(slot).wait_recv()
    for place, slot in enumerate(soon):
        take(slot, place)
    edges_near, cells_near = edges + near * halo_edges, cells + near * halo_cells
    tangent_sum[...] += tangent_part(edges, edges_near)
    average_sum[...] += average_part(cells, cells_near)

    slow = [2 * lax.rem(final + 1 + place, reach) + parity for place in range(reach)]
    edges_late, cells_late = edges_near + 2 * halo_edges, cells_near + 2 * halo_cells
    for slot in slow[:2]:
        copy_of(slot).wait_recv()
    for place in range(2):
        take(slow[place], near + place)
    tangent_sum[...] += tangent_part(edges_near, edges_late)
    average_sum[...] += average_part(cells_near, cells_late)

    copy_of(slow[2]).wait_recv()
    take(slow[2], near + 2)
    averaged = average_sum[...] + average_part(cells_late, density_ext.shape[1])
    wind = wind_ext[...]
    fluxes = halves(jnp.concatenate([wind, wind], axis=0) * averaged)
    both = dot(fluxes, diverge[...])
    divergence = both[0 : 2 * padded] + both[2 * padded :] + dot(
        fluxes[0 : 2 * padded], diverge_trail[...]
    )
    tend_ref[...] = -divergence[0:levels]
    values[...] = (theta_ext[:, 0:cells] - STEP_SIZE * divergence[padded:])
    values[0:levels, :] = values[0:levels, :] * inverse[0:levels, :]

    tangential = tangent_sum[...] + tangent_part(edges_late, wind_ext.shape[1])
    tangential_ref[...] = tangential[0:levels]

    def row(ref, level):
        return ref[level : level + 1, :]

    upward, downward = none, none
    for step in range(max(middle, levels - 1 - middle)):
        if step < middle:
            upward = row(values, step) + row(carried, step) * upward
            values[step : step + 1, :] = upward
        level = levels - 1 - step
        if level > middle:
            downward = row(values, level) + row(carried, level) * downward
            values[level : level + 1, :] = downward
    upward = (
        row(values, middle) + row(carried, middle) * upward + row(ratios, middle) * downward
    )
    theta_new_ref[middle : middle + 1, :] = upward
    downward = upward
    for step in range(1, max(middle, levels - 1 - middle) + 1):
        if middle - step >= 0:
            upward = row(values, middle - step) + row(ratios, middle - step) * upward
            theta_new_ref[middle - step : middle - step + 1, :] = upward
        level = middle + step
        if level < levels:
            downward = row(values, level) + row(ratios, level) * downward
            theta_new_ref[level : level + 1, :] = downward
    for slot in SEND_ORDER:
        copy_of(slot).wait_send()


def deliver(*refs):
    sources, targets, store_sem = refs[:3], refs[3:6], refs[6]
    stores = [
        pltpu.make_async_copy(source, target_ref.at[:, 0, :], store_sem.at[n])
        for n, (source, target_ref) in enumerate(zip(sources, targets))
    ]
    for store in stores:
        store.start()
    for store in stores:
        store.wait()


def shards(*arguments):
    wind, density, theta, cell_edges, edge_cells, edges_on_edge, send_cells, send_edges = arguments[:8]
    levels, edges = wind.shape[1:]
    cells = density.shape[2]
    slots, halo_cells = send_cells.shape[1:]
    halo_edges = send_edges.shape[2]
    padded = -(-levels // 8) * 8
    edges_ext = edge_cells.shape[2]
    cells_ext = -(-(cells + slots * halo_cells) // LANES) * LANES
    landed = [*arguments[:3], cell_edges, edge_cells, edges_on_edge, send_cells, send_edges, *arguments[8:]]
    operands = [x if x is edge_cells else jnp.transpose(x, (1, 0, 2)) for x in arguments]
    hbm = pl.BlockSpec(memory_space=pl.ANY)
    vmem = pl.BlockSpec(memory_space=pltpu.VMEM)
    widths = (cells, cells, edges)
    results = pl.pallas_call(
        kernel,
        out_shape=tuple(pltpu.VMEM((levels, width), F32) for width in widths),
        in_specs=[hbm] * len(arguments),
        out_specs=(vmem,) * 3,
        scratch_shapes=[
            *(pltpu.VMEM(x.shape[1:], x.dtype) for x in landed),
            pltpu.VMEM((padded, edges_ext), F32),
            pltpu.VMEM((padded, cells_ext), F32),
            pltpu.VMEM((padded, cells_ext), F32),
            pltpu.VMEM((slots, padded, 2 * halo_cells + halo_edges), F32),
            pltpu.VMEM((slots, padded, 2 * halo_cells + halo_edges), F32),
            pltpu.VMEM((cells_ext, edges_ext), BF16),
            pltpu.VMEM(edge_cells.shape[1:], F32),
            pltpu.VMEM((edges_ext, cells), BF16),
            pltpu.VMEM((edges_ext, cells), BF16),
            pltpu.VMEM(cell_edges.shape[1:], F32),
            pltpu.VMEM((edges_ext, edges), BF16),
            pltpu.VMEM((edges_ext, edges), BF16),
            pltpu.VMEM(edges_on_edge.shape[1:], F32),
            pltpu.VMEM((2 * padded, edges_ext), F32),
            pltpu.VMEM((padded, edges), F32),
            pltpu.VMEM((padded, cells), F32),
            pltpu.VMEM((padded, cells), F32),
            pltpu.VMEM((padded, cells), F32),
            pltpu.VMEM((padded, cells), F32),
            pltpu.SemaphoreType.DMA((slots,)),
            pltpu.SemaphoreType.DMA((len(arguments),)),
            pltpu.SemaphoreType.REGULAR,
            pltpu.SemaphoreType.REGULAR,
        ],
        compiler_params=pltpu.CompilerParams(collective_id=0, has_side_effects=True),
    )(*operands)
    results = pl.pallas_call(
        deliver,
        out_shape=tuple(jax.ShapeDtypeStruct((levels, 1, width), F32) for width in widths),
        in_specs=[vmem] * 3,
        out_specs=(hbm,) * 3,
        scratch_shapes=[pltpu.SemaphoreType.DMA((3,))],
    )(*(pltpu.with_memory_space_constraint(x, pltpu.VMEM) for x in results))
    return tuple(jnp.transpose(x, (1, 0, 2)) for x in results)


def solution(mesh):
    placed = P(("blk", "sub"), None, None)
    return jax.shard_map(
        shards,
        mesh=mesh,
        in_specs=(placed,) * 11,
        out_specs=(placed,) * 3,
        check_vma=False,
    )
```
